32 devices in a mesh: pairs: 8 (over y, x, core), aux: 4 (over z).
Axes of the slice: x: 2, y: 2, z: 4, core: 2. Of those that a mesh axis runs over, the one named last changes fastest.
Arguments:
- panels: bfloat16 [64, 3584, 256], P(None, ('pairs', 'aux')), may hold values from -0.59765625 to 0.59765625
- domain: int32 [8, 6], replicated, may hold values from 0 to 63, as said below
- pair_slots: int32 [96, 2], P('pairs'), may hold values from 0 to 5
- ranks: int32 [96, 2], P('pairs'), may hold values from 40 to 128
- transforms: bfloat16 [96, 2, 256, 128], P('pairs'), may hold values from -0.375 to 0.375
- trial: bfloat16 [96, 2, 128, 128], P('pairs'), may hold values from -0.5 to 0.5
Outputs:
- sigma: bfloat16 [96, 2, 128, 128], P('pairs', None, 'aux')
The draws below stay inside these ranges and needn't reach their ends.
Inputs may be any that keep to these rules, and one draw needn't show every extreme that they name: `domain`: each row holds 6 different LMO numbers.
All inputs are finite; a program needn't handle non-finite values.
Results may differ from the reference program's by a relative error of at most 0.0039.
Values may be sent and summed in bfloat16 or wider, within the bound.
A program may use at most 128 MiB of HBM per device.

```python
import jax
import jax.numpy as jnp
from jax import lax

NV = 256
R = 128
ROOTS = 2
NOCC = 64
LSLOT = 6
PAIR_DEV = 12
NAUX = 3584
GROUPS = 8
PAIRS = 96


def draw_domain(key, part):
    keys = jax.random.split(jax.random.fold_in(key, 11), GROUPS)
    rows = jax.vmap(lambda single: jax.random.permutation(single, NOCC)[:LSLOT])(keys)
    return rows.astype(jnp.int32)


def place_ends(drawn, stream_key, smallest, largest):
    longest = drawn.shape.index(max(drawn.shape))
    spots = []
    for shift in (0, 1):
        where = [jax.random.randint(jax.random.fold_in(stream_key, axis), (), 0, length) for axis, length in enumerate(drawn.shape)]
        where[longest] = (where[longest] + shift) % drawn.shape[longest]
        spots.append(tuple(where))
    return drawn.at[spots[0]].set(smallest).at[spots[1]].set(largest)


def steps_of(rng, shape, cuts, least, largest):
    gain, own = 1.0, jax.random.fold_in(rng, 6)
    for axis_at, parts in cuts:
        draws = jnp.exp(jax.random.uniform(jax.random.fold_in(own, axis_at), (parts,), jnp.float32, least / len(cuts), largest / len(cuts)))
        gain = gain * jnp.repeat(draws, shape[axis_at] // parts).reshape([-1 if axis == axis_at else 1 for axis in range(len(shape))])
    return gain


def normal_values(rng, extent, deviation, reach, cuts=(), held_as=jnp.bfloat16):
    values = deviation * jax.random.normal(rng, extent, jnp.float32)
    if cuts:
        values = values * steps_of(rng, extent, cuts, -0.22, 0.18)
    return jnp.clip(values, -reach, reach).astype(held_as)


def setup_inputs(seed: int = 0) -> dict:
    key_of = jax.random.split(jax.random.key(seed), 7)
    panels = normal_values(key_of[0], (NOCC, NAUX, NV), 0.08, 0.59765625, ((1, 32),))
    domain = draw_domain(jax.random.fold_in(key_of[6], 71), 0)
    pair_slots = place_ends(jax.random.randint(key_of[2], (PAIRS, 2), 0, LSLOT), jax.random.fold_in(key_of[2], 1), 0, LSLOT - 1).astype(jnp.int32)
    ranks = place_ends(jax.random.randint(key_of[3], (PAIRS, ROOTS), R * 5 // 16, R + 1), jax.random.fold_in(key_of[3], 1), R * 5 // 16, R).astype(jnp.int32)
    transforms = normal_values(key_of[4], (PAIRS, ROOTS, NV, R), NV ** -0.5, 0.375, ((0, 8),))
    trial = normal_values(key_of[5], (PAIRS, ROOTS, R, R), R ** -0.5, 0.5, ((0, 8),))
    return {"panels": panels, "domain": domain, "pair_slots": pair_slots, "ranks": ranks, "transforms": transforms, "trial": trial}


def reference(panels, domain, pair_slots, ranks, transforms, trial):
    positions = jnp.arange(R, dtype=jnp.int32)

    def one_pair(index):
        group = index // PAIR_DEV
        lmo_ids = domain[group][pair_slots[index]]
        left = panels[lmo_ids[0]].astype(jnp.float32)
        right = panels[lmo_ids[1]].astype(jnp.float32)
        keep = (positions[None, :] < ranks[index][:, None]).astype(jnp.float32)
        coeffs = transforms[index].astype(jnp.float32) * keep[:, None, :]
        amplitude = trial[index].astype(jnp.float32) * keep[:, :, None] * keep[:, None, :]
        left_proj = jnp.einsum('qv,svr->sqr', left, coeffs, precision=lax.Precision.HIGHEST).astype(jnp.bfloat16)
        right_proj = jnp.einsum('qv,svr->sqr', right, coeffs, precision=lax.Precision.HIGHEST).astype(jnp.bfloat16)
        left_proj, right_proj = lax.optimization_barrier((left_proj, right_proj))
        kmat = jnp.einsum('sqa,sqb->sab', left_proj.astype(jnp.float32), right_proj.astype(jnp.float32), precision=lax.Precision.HIGHEST)
        with_right = jnp.einsum('sab,sbc->sac', kmat, amplitude, precision=lax.Precision.HIGHEST)
        with_left = jnp.einsum('sac,sbc->sab', amplitude, kmat, precision=lax.Precision.HIGHEST)
        return (kmat + with_right + with_left).astype(jnp.bfloat16)

    return lax.map(one_pair, jnp.arange(PAIRS, dtype=jnp.int32))
```

```python
import functools

import jax
import jax.numpy as jnp
from jax import lax
from jax.experimental import pallas as pl
from jax.experimental.pallas import tpu as pltpu
from jax.sharding import PartitionSpec as P

MESH = pl.DeviceIdType.MESH
CORES = 2


def peer_of(me, offset, count):
    if count & (count - 1):
        return lax.rem(me + offset, count)
    peer = me
    bit = 1
    while bit < count:
        if offset & bit:
            peer = peer + bit * (1 - 2 * lax.rem(me // bit, 2))
        bit *= 2
    return peer


def complete_after(slots, pairs):
    sure = pairs
    counts = [pairs]
    for left in range(slots, 1, -1):
        sure -= min(sure, 2 * sure // left)
        counts.insert(0, sure)
    return counts


def elimination(slots_ref, slots, pairs):
    bits = (pairs + 1).bit_length()
    left = [slots_ref[0, pair] for pair in range(pairs)]
    right = [slots_ref[1, pair] for pair in range(pairs)]
    fields = 31 // bits
    words = -(-slots // fields)

    def mark(slot, word):
        low = word * fields
        shift = slot - low
        inside = (shift >= 0) & (shift < fields)
        return jnp.where(inside, jnp.left_shift(1, jnp.where(inside, shift, 0) * bits), 0)

    marks = [[mark(left[p], w) | mark(right[p], w) for w in range(words)] for p in range(pairs)]
    alive = [jnp.int32(1)] * pairs
    rank = [jnp.int32(0)] * pairs
    place = [jnp.int32(0)] * slots
    taken = [jnp.int32(0)] * slots
    for spot in range(slots - 1, -1, -1):
        totals = [sum(alive[p] * marks[p][w] for p in range(pairs)) for w in range(words)]
        best, pick = None, None
        for slot in range(slots):
            count = (totals[slot // fields] >> (bits * (slot % fields))) & (2**bits - 1)
            count = count + taken[slot] * 2**bits
            if best is None:
                best, pick = count, jnp.int32(slot)
            else:
                less = count < best
                best = jnp.where(less, count, best)
                pick = jnp.where(less, slot, pick)
        for slot in range(slots):
            hit = pick == slot
            place[slot] = jnp.where(hit, spot, place[slot])
            taken[slot] = jnp.where(hit, 1, taken[slot])
        gone = []
        for p in range(pairs):
            touch = (left[p] == pick) | (right[p] == pick)
            gone.append(jnp.where(touch, alive[p], 0))
            alive[p] = alive[p] - gone[p]
        at = sum(alive)
        for p in range(pairs):
            rank[p] = jnp.where(gone[p] == 1, at, rank[p])
            at = at + gone[p]
    return place, rank


def fused_kernel(
    n, m, domain_ref, slots_ref, ranks_ref, panels_ref, d_ref, c_ref, out_ref,
    panels, outgoing, recv, block, d_raw, d_mask, c_raw, acc, send_buf, landed, total,
    place_ref, rank_ref, perm_ref, mine_order, orders,
    local_sem, send_sem, recv_sem, order_send, order_recv, part_send, part_recv,
):
    me = lax.axis_index("pairs")
    mine = lax.axis_index("aux")
    core = lax.rem(me, CORES)
    chip = me // CORES
    chips = n // CORES
    pairs, roots, nv, width = d_ref.shape
    slots = domain_ref.shape[1]
    rows = panels_ref.shape[1]
    strip = width // m
    sure = complete_after(slots, pairs)
    last = CORES - 1

    def device(k, dest):
        return peer_of(chip, k, chips) * CORES + dest

    barrier = pltpu.get_barrier_semaphore()
    for k in range(chips):
        for dest in range(CORES):
            if k:
                pl.semaphore_signal(barrier, inc=1, device_id=(device(k, dest), mine), device_id_type=MESH)
    pl.semaphore_signal(barrier, inc=1, device_id=(chip * CORES + 1 - core, mine), device_id_type=MESH)
    for offset in range(1, m):
        pl.semaphore_signal(barrier, inc=1, device_id=(me, lax.rem(mine + offset, m)), device_id_type=MESH)
    panels_copy = pltpu.make_async_copy(panels_ref, panels, local_sem.at[0])
    panels_copy.start()
    d_copy = pltpu.make_async_copy(d_ref, d_raw, local_sem.at[1])
    d_copy.start()
    c_copy = pltpu.make_async_copy(c_ref, c_raw, local_sem.at[2])
    c_copy.start()

    place, rank = elimination(slots_ref, slots, pairs)
    for slot in range(slots):
        place_ref[slot] = jnp.where(core == last, place[slot], slot)
    for pair in range(pairs):
        rank_ref[pair] = rank[pair]
    for spot in range(slots):
        chosen = sum(jnp.where(place[slot] == spot, slot, 0) for slot in range(slots))
        mine_order[0, spot] = jnp.where(core == last, chosen, spot)
    for q in range(pairs):
        perm_ref[q] = sum(jnp.where(rank[pair] == q, pair, 0) for pair in range(pairs))

    pl.semaphore_wait(barrier, n + m - 2)

    def order_copy(peer, k, slot):
        return pltpu.make_async_remote_copy(
            src_ref=mine_order,
            dst_ref=orders.at[slot],
            send_sem=order_send.at[k],
            recv_sem=order_recv.at[slot],
            device_id=(peer, mine),
            device_id_type=MESH,
        )

    @pl.when(core == last)
    def _():
        for k in range(1, chips):
            for dest in range(CORES):
                order_copy(device(k, dest), k * CORES + dest, chip).start()
        order_copy(chip * CORES, 0, chip).start()

    panels_copy.wait()

    def panel_copy(k, dest, spot):
        return pltpu.make_async_remote_copy(
            src_ref=outgoing.at[dest, k, spot],
            dst_ref=recv.at[spot, k * CORES + core],
            send_sem=send_sem.at[dest, k, spot],
            recv_sem=recv_sem.at[spot, k * CORES + core],
            device_id=(device(k, dest), mine),
            device_id_type=MESH,
        )

    def send_all(dest, slot_of):
        waiting = None
        for spot in range(slots):
            for k in range(1, chips):
                peer = device(k, dest)
                outgoing[dest, k, spot] = panels[domain_ref[peer, slot_of(k, spot)]]
                if waiting is not None:
                    waiting.start()
                waiting = panel_copy(k, dest, spot)
        peer = chip * CORES + dest
        for spot in range(slots):
            outgoing[dest, 0, spot] = panels[domain_ref[peer, slot_of(0, spot)]]
        waiting.start()

        @pl.when(core != dest)
        def _():
            for spot in range(slots):
                panel_copy(0, dest, spot).start()

        @pl.when(core == dest)
        def _():
            for spot in range(slots):
                recv[spot, dest] = outgoing[dest, 0, spot]

    for dest in range(last):
        send_all(dest, lambda k, spot: spot)

    for k in range(1, chips):
        slot = peer_of(chip, k, chips)
        order_copy(chip * CORES, 0, slot).wait_recv()

    @pl.when(core != last)
    def _():
        order_copy(chip * CORES, 0, chip).wait_recv()

    @pl.when(core == last)
    def _():
        for spot in range(slots):
            orders[chip, 0, spot] = mine_order[0, spot]

    send_all(last, lambda k, spot: orders[peer_of(chip, k, chips), 0, spot])

    columns = lax.broadcasted_iota(jnp.int32, (1, width), 1)
    row_ids = lax.broadcasted_iota(jnp.int32, (width, 1), 0)
    d_copy.wait()
    c_copy.wait()

    def mask_pair(pair, carry):
        for root in range(roots):
            limit = ranks_ref[root, pair]
            d_mask[pair, :, root * width:(root + 1) * width] = jnp.where(
                columns < limit, d_raw[pair, root], jnp.zeros((), d_raw.dtype)
            )
            keep = (columns < limit) & (row_ids < limit)
            c_raw[pair, root] = jnp.where(keep, c_raw[pair, root], jnp.zeros((), c_raw.dtype))
        return carry

    lax.fori_loop(0, pairs, mask_pair, 0)

    def part_copy(q, offset):
        peer = lax.rem(mine + offset, m)
        return pltpu.make_async_remote_copy(
            src_ref=send_buf.at[peer, q],
            dst_ref=landed.at[offset - 1, q],
            send_sem=part_send.at[q, offset],
            recv_sem=part_recv.at[q, offset],
            device_id=(me, peer),
            device_id_type=MESH,
        )

    def compute(q, carry):
        pair = perm_ref[q]
        coeffs = d_mask[pair]
        left = block[place_ref[slots_ref[0, pair]]]
        right = block[place_ref[slots_ref[1, pair]]]
        left = jnp.dot(left, coeffs, preferred_element_type=jnp.float32).astype(jnp.bfloat16)
        right = jnp.dot(right, coeffs, preferred_element_type=jnp.float32).astype(jnp.bfloat16)
        for root in range(roots):
            kmat = lax.dot_general(
                left[:, root * width:(root + 1) * width],
                right[:, root * width:(root + 1) * width],
                (((0,), (0,)), ((), ())),
                preferred_element_type=jnp.float32,
            )
            rounded = kmat.astype(jnp.bfloat16)
            amplitude = c_raw[pair, root]
            with_right = jnp.dot(rounded, amplitude, preferred_element_type=jnp.float32)
            with_left = lax.dot_general(
                amplitude, rounded, (((1,), (1,)), ((), ())), preferred_element_type=jnp.float32
            )
            sigma = kmat + with_right + with_left
            acc[q, root] = sigma
            for owner in range(m):
                send_buf[owner, q, root] = sigma[owner * strip:(owner + 1) * strip].astype(jnp.bfloat16)
        for offset in range(1, m):
            part_copy(q, offset).start()
        return carry

    def take(spot):
        for lane in range(n):
            if lane < CORES:

                @pl.when(core != lane)
                def _():
                    arrived(lane, spot).wait_recv()

            else:
                arrived(lane, spot).wait_recv()
        block[spot] = recv[spot].reshape(n * rows, nv)

    def arrived(lane, spot):
        return pltpu.make_async_remote_copy(
            src_ref=outgoing.at[0, 0, spot],
            dst_ref=recv.at[spot, lane],
            send_sem=send_sem.at[0, 0, spot],
            recv_sem=recv_sem.at[spot, lane],
            device_id=(chip * CORES + 1 - core, mine),
            device_id_type=MESH,
        )

    @pl.when(core != last)
    def _():
        for spot in range(slots):
            take(spot)

    done = 0
    for spot in range(slots):

        @pl.when(core == last)
        def _():
            take(spot)

        if sure[spot] > done:
            lax.fori_loop(done, sure[spot], compute, 0)
            done = sure[spot]

    for q in range(pairs):
        for offset in range(1, m):
            part_copy(q, offset).wait_recv()
        value = acc[q, :, pl.ds(pl.multiple_of(mine * strip, strip), strip), :]
        for offset in range(1, m):
            value = value + landed[offset - 1, q].astype(jnp.float32)
        total[q] = value.astype(total.dtype)
    for pair in range(pairs):
        out_ref[pair] = total[rank_ref[pair]]

    for dest in range(CORES):
        for spot in range(slots):
            for k in range(1, chips):
                panel_copy(k, dest, spot).wait_send()

        @pl.when(core != dest)
        def _():
            for spot in range(slots):
                panel_copy(0, dest, spot).wait_send()

    @pl.when(core == last)
    def _():
        for k in range(1, chips):
            for dest in range(CORES):
                order_copy(device(k, dest), k * CORES + dest, chip).wait_send()
        order_copy(chip * CORES, 0, chip).wait_send()

    for q in range(pairs):
        for offset in range(1, m):
            part_copy(q, offset).wait_send()


def per_device(n, m, panels, domain, pair_slots, ranks, transforms, trial):
    pairs, roots, nv, width = transforms.shape
    slots = domain.shape[1]
    rows = panels.shape[1]
    chips = n // CORES
    strip = width // m
    bf16 = jnp.bfloat16
    smem = pl.BlockSpec(memory_space=pltpu.SMEM)
    hbm = pl.BlockSpec(memory_space=pltpu.HBM)
    dma = pltpu.SemaphoreType.DMA
    return pl.pallas_call(
        functools.partial(fused_kernel, n, m),
        in_specs=[smem, smem, smem, hbm, hbm, hbm],
        out_specs=pl.BlockSpec(memory_space=pltpu.VMEM),
        out_shape=jax.ShapeDtypeStruct((pairs, roots, strip, width), bf16),
        scratch_shapes=[
            pltpu.VMEM(panels.shape, bf16),
            pltpu.VMEM((CORES, chips, slots, rows, nv), bf16),
            pltpu.VMEM((slots, n, rows, nv), bf16),
            pltpu.VMEM((slots, n * rows, nv), bf16),
            pltpu.VMEM((pairs, roots, nv, width), bf16),
            pltpu.VMEM((pairs, nv, roots * width), bf16),
            pltpu.VMEM((pairs, roots, width, width), bf16),
            pltpu.VMEM((pairs, roots, width, width), jnp.float32),
            pltpu.VMEM((m, pairs, roots, strip, width), bf16),
            pltpu.VMEM((m - 1, pairs, roots, strip, width), bf16),
            pltpu.VMEM((pairs, roots, strip, width), bf16),
            pltpu.SMEM((slots,), jnp.int32),
            pltpu.SMEM((pairs,), jnp.int32),
            pltpu.SMEM((pairs,), jnp.int32),
            pltpu.SMEM((1, 128), jnp.int32),
            pltpu.SMEM((chips, 1, 128), jnp.int32),
            dma((3,)),
            dma((CORES, chips, slots)),
            dma((slots, n)),
            dma((n,)),
            dma((chips,)),
            dma((pairs, m)),
            dma((pairs, m)),
        ],
        compiler_params=pltpu.CompilerParams(
            collective_id=0, has_side_effects=True, vmem_limit_bytes=60 * 2**20
        ),
    )(domain, pair_slots.T, ranks.T, panels, transforms, trial)


def solution(mesh):
    return jax.shard_map(
        functools.partial(per_device, mesh.shape["pairs"], mesh.shape["aux"]),
        mesh=mesh,
        in_specs=(
            P(None, ("pairs", "aux"), None),
            P(),
            P("pairs", None),
            P("pairs", None),
            P("pairs", None, None, None),
            P("pairs", None, None, None),
        ),
        out_specs=P("pairs", None, "aux", None),
        check_vma=False,
    )
```

```python
import functools

import jax
import jax.numpy as jnp
from jax import lax
from jax.experimental import pallas as pl
from jax.experimental.pallas import tpu as pltpu
from jax.sharding import PartitionSpec as P

MESH = pl.DeviceIdType.MESH
CORES = 2


def peer_of(me, offset, count):
    if count & (count - 1):
        return lax.rem(me + offset, count)
    peer = me
    bit = 1
    while bit < count:
        if offset & bit:
            peer = peer + bit * (1 - 2 * lax.rem(me // bit, 2))
        bit *= 2
    return peer


def complete_after(slots, pairs):
    sure = pairs
    counts = [pairs]
    for left in range(slots, 1, -1):
        sure -= min(sure, 2 * sure // left)
        counts.insert(0, sure)
    return counts


def elimination(slots_ref, slots, pairs):
    bits = (pairs + 1).bit_length()
    left = [slots_ref[0, pair] for pair in range(pairs)]
    right = [slots_ref[1, pair] for pair in range(pairs)]
    fields = 31 // bits
    words = -(-slots // fields)

    def mark(slot, word):
        low = word * fields
        shift = slot - low
        inside = (shift >= 0) & (shift < fields)
        return jnp.where(inside, jnp.left_shift(1, jnp.where(inside, shift, 0) * bits), 0)

    marks = [[mark(left[p], w) | mark(right[p], w) for w in range(words)] for p in range(pairs)]
    alive = [jnp.int32(1)] * pairs
    rank = [jnp.int32(0)] * pairs
    place = [jnp.int32(0)] * slots
    taken = [jnp.int32(0)] * slots
    for spot in range(slots - 1, -1, -1):
        totals = [sum(alive[p] * marks[p][w] for p in range(pairs)) for w in range(words)]
        best, pick = None, None
        for slot in range(slots):
            count = (totals[slot // fields] >> (bits * (slot % fields))) & (2**bits - 1)
            count = count + taken[slot] * 2**bits
            if best is None:
                best, pick = count, jnp.int32(slot)
            else:
                less = count < best
                best = jnp.where(less, count, best)
                pick = jnp.where(less, slot, pick)
        for slot in range(slots):
            hit = pick == slot
            place[slot] = jnp.where(hit, spot, place[slot])
            taken[slot] = jnp.where(hit, 1, taken[slot])
        gone = []
        for p in range(pairs):
            touch = (left[p] == pick) | (right[p] == pick)
            gone.append(jnp.where(touch, alive[p], 0))
            alive[p] = alive[p] - gone[p]
        at = sum(alive)
        for p in range(pairs):
            rank[p] = jnp.where(gone[p] == 1, at, rank[p])
            at = at + gone[p]
    return place, rank


def fused_kernel(
    n, m, domain_ref, slots_ref, ranks_ref, panels_ref, d_ref, c_ref, out_ref,
    panels, outgoing, recv, block, d_raw, d_mask, c_raw, acc, send_buf, landed, total,
    place_ref, rank_ref, perm_ref, mine_order, orders,
    local_sem, send_sem, recv_sem, order_sem, part_send, part_recv, from_below, from_above,
):
    me = lax.axis_index("pairs")
    mine = lax.axis_index("aux")
    core = lax.rem(me, CORES)
    chip = me // CORES
    chips = n // CORES
    pairs, roots, nv, width = d_ref.shape
    slots = domain_ref.shape[1]
    rows = panels_ref.shape[1]
    strip = width // m
    sure = complete_after(slots, pairs)
    last = CORES - 1
    early = sure[-2] - 1

    def device(k, dest):
        return peer_of(chip, k, chips) * CORES + dest

    barrier = pltpu.get_barrier_semaphore()
    for k in range(chips):
        for dest in range(CORES):
            if k:
                pl.semaphore_signal(barrier, inc=1, device_id=(device(k, dest), mine), device_id_type=MESH)
    pl.semaphore_signal(barrier, inc=1, device_id=(chip * CORES + 1 - core, mine), device_id_type=MESH)

    @pl.when(mine > 0)
    def _():
        pl.semaphore_signal(barrier, inc=1, device_id=(me, mine - 1), device_id_type=MESH)

    @pl.when(mine < m - 1)
    def _():
        pl.semaphore_signal(barrier, inc=1, device_id=(me, mine + 1), device_id_type=MESH)

    panels_copy = pltpu.make_async_copy(panels_ref, panels, local_sem.at[0])
    panels_copy.start()
    d_copy = pltpu.make_async_copy(d_ref, d_raw, local_sem.at[1])
    d_copy.start()
    c_copy = pltpu.make_async_copy(c_ref, c_raw, local_sem.at[2])
    c_copy.start()

    place, rank = elimination(slots_ref, slots, pairs)
    for slot in range(slots):
        place_ref[slot] = jnp.where(core == last, place[slot], slot)
    for pair in range(pairs):
        rank_ref[pair] = rank[pair]
    for spot in range(slots):
        chosen = sum(jnp.where(place[slot] == spot, slot, 0) for slot in range(slots))
        mine_order[0, spot] = jnp.where(core == last, chosen, spot)
    for q in range(pairs):
        perm_ref[q] = sum(jnp.where(rank[pair] == q, pair, 0) for pair in range(pairs))

    beside = jnp.where(mine > 0, 1, 0) + jnp.where(mine < m - 1, 1, 0)
    pl.semaphore_wait(barrier, n - 1 + beside)

    def order_copy(peer):
        return pltpu.make_async_remote_copy(
            src_ref=mine_order,
            dst_ref=orders.at[chip],
            send_sem=order_sem.at[0],
            recv_sem=order_sem.at[1],
            device_id=(peer, mine),
            device_id_type=MESH,
        )

    @pl.when(core == last)
    def _():
        for k in range(1, chips):
            for dest in range(CORES):
                order_copy(device(k, dest)).start()
        order_copy(chip * CORES).start()

    panels_copy.wait()

    def panel_copy(k, dest, spot):
        return pltpu.make_async_remote_copy(
            src_ref=outgoing.at[dest, k, spot],
            dst_ref=recv.at[spot, k * CORES + core],
            send_sem=send_sem,
            recv_sem=recv_sem.at[spot],
            device_id=(device(k, dest), mine),
            device_id_type=MESH,
        )

    def send_all(dest, slot_of):
        waiting = None
        for spot in range(slots):
            for k in range(1, chips):
                peer = device(k, dest)
                outgoing[dest, k, spot] = panels[domain_ref[peer, slot_of(k, spot)]]
                if waiting is not None:
                    waiting.start()
                waiting = panel_copy(k, dest, spot)
        peer = chip * CORES + dest
        for spot in range(slots):
            outgoing[dest, 0, spot] = panels[domain_ref[peer, slot_of(0, spot)]]
        waiting.start()

        @pl.when(core != dest)
        def _():
            for spot in range(slots):
                panel_copy(0, dest, spot).start()

        @pl.when(core == dest)
        def _():
            for spot in range(slots):
                recv[spot, dest] = outgoing[dest, 0, spot]

    for dest in range(last):
        send_all(dest, lambda k, spot: spot)

    def orders_done(sem, count):
        whole = orders.at[pl.ds(0, count)]
        pltpu.make_async_copy(whole, whole, order_sem.at[sem]).wait()

    @pl.when(core != last)
    def _():
        orders_done(1, chips)

    @pl.when(core == last)
    def _():
        orders_done(1, chips - 1)

    @pl.when(core == last)
    def _():
        for spot in range(slots):
            orders[chip, 0, spot] = mine_order[0, spot]

    send_all(last, lambda k, spot: orders[peer_of(chip, k, chips), 0, spot])

    for far in range(2, m):

        @pl.when((mine >= far - 1) & (mine < m - 1))
        def _():
            pl.semaphore_signal(from_below, inc=1, device_id=(me, mine + 1), device_id_type=MESH)

        @pl.when((mine <= m - far) & (mine > 0))
        def _():
            pl.semaphore_signal(from_above, inc=1, device_id=(me, mine - 1), device_id_type=MESH)

        @pl.when(mine >= far)
        def _():
            pl.semaphore_wait(from_below, 1)

        @pl.when(mine < m - far)
        def _():
            pl.semaphore_wait(from_above, 1)

    columns = lax.broadcasted_iota(jnp.int32, (1, width), 1)
    row_ids = lax.broadcasted_iota(jnp.int32, (width, 1), 0)
    d_copy.wait()
    c_copy.wait()

    def mask_pair(pair, carry):
        for root in range(roots):
            limit = ranks_ref[root, pair]
            d_mask[pair, :, root * width:(root + 1) * width] = jnp.where(
                columns < limit, d_raw[pair, root], jnp.zeros((), d_raw.dtype)
            )
            keep = (columns < limit) & (row_ids < limit)
            c_raw[pair, root] = jnp.where(keep, c_raw[pair, root], jnp.zeros((), c_raw.dtype))
        return carry

    lax.fori_loop(0, pairs, mask_pair, 0)

    def part_copy(q, offset):
        peer = lax.rem(mine + offset, m)
        return pltpu.make_async_remote_copy(
            src_ref=send_buf.at[peer, q],
            dst_ref=landed.at[offset - 1, q],
            send_sem=part_send,
            recv_sem=part_recv.at[jnp.maximum(q - early, 0)],
            device_id=(me, peer),
            device_id_type=MESH,
        )

    def compute(q, carry):
        pair = perm_ref[q]
        coeffs = d_mask[pair]
        left = block[place_ref[slots_ref[0, pair]]]
        right = block[place_ref[slots_ref[1, pair]]]
        left = jnp.dot(left, coeffs, preferred_element_type=jnp.float32).astype(jnp.bfloat16)
        right = jnp.dot(right, coeffs, preferred_element_type=jnp.float32).astype(jnp.bfloat16)
        for root in range(roots):
            kmat = lax.dot_general(
                left[:, root * width:(root + 1) * width],
                right[:, root * width:(root + 1) * width],
                (((0,), (0,)), ((), ())),
                preferred_element_type=jnp.float32,
            )
            rounded = kmat.astype(jnp.bfloat16)
            amplitude = c_raw[pair, root]
            with_right = jnp.dot(rounded, amplitude, preferred_element_type=jnp.float32)
            with_left = lax.dot_general(
                amplitude, rounded, (((1,), (1,)), ((), ())), preferred_element_type=jnp.float32
            )
            sigma = kmat + with_right + with_left
            acc[q, root] = sigma
            for owner in range(m):
                send_buf[owner, q, root] = sigma[owner * strip:(owner + 1) * strip].astype(jnp.bfloat16)
        for offset in range(1, m):
            part_copy(q, offset).start()
        return carry

    def take(spot):
        others = recv.at[spot, pl.ds(0, n - 1)]
        pltpu.make_async_copy(others, others, recv_sem.at[spot]).wait()
        block[spot] = recv[spot].reshape(n * rows, nv)

    @pl.when(core != last)
    def _():
        for spot in range(slots):
            take(spot)

    done = 0
    for spot in range(slots):

        @pl.when(core == last)
        def _():
            take(spot)

        if sure[spot] > done:
            lax.fori_loop(done, sure[spot], compute, 0)
            done = sure[spot]

    gone = outgoing.at[:, pl.ds(1, chips - 1)]
    pltpu.make_async_copy(gone, gone, send_sem).wait()
    gone = outgoing.at[0, 0]
    pltpu.make_async_copy(gone, gone, send_sem).wait()

    @pl.when(core == last)
    def _():
        for _ in range(n - 1):
            orders_done(0, 1)

    def sum_of(q):
        value = acc[q, :, pl.ds(pl.multiple_of(mine * strip, strip), strip), :]
        for offset in range(1, m):
            value = value + landed[offset - 1, q].astype(jnp.float32)
        total[q] = value.astype(total.dtype)

    lots = landed.at[:, pl.ds(0, early + 1)]
    pltpu.make_async_copy(lots, lots, part_recv.at[0]).wait()
    for q in range(early + 1):
        sum_of(q)
    for q in range(early + 1, pairs):
        lot = landed.at[:, q]
        pltpu.make_async_copy(lot, lot, part_recv.at[q - early]).wait()
        sum_of(q)
    for pair in range(pairs):
        out_ref[pair] = total[rank_ref[pair]]
    sent = send_buf.at[pl.ds(0, m - 1)]
    pltpu.make_async_copy(sent, sent, part_send).wait()


def per_device(n, m, panels, domain, pair_slots, ranks, transforms, trial):
    pairs, roots, nv, width = transforms.shape
    slots = domain.shape[1]
    rows = panels.shape[1]
    chips = n // CORES
    strip = width // m
    bf16 = jnp.bfloat16
    smem = pl.BlockSpec(memory_space=pltpu.SMEM)
    hbm = pl.BlockSpec(memory_space=pltpu.HBM)
    dma = pltpu.SemaphoreType.DMA
    return pl.pallas_call(
        functools.partial(fused_kernel, n, m),
        in_specs=[smem, smem, smem, hbm, hbm, hbm],
        out_specs=pl.BlockSpec(memory_space=pltpu.VMEM),
        out_shape=pltpu.VMEM((pairs, roots, strip, width), bf16),
        scratch_shapes=[
            pltpu.VMEM(panels.shape, bf16),
            pltpu.VMEM((CORES, chips, slots, rows, nv), bf16),
            pltpu.VMEM((slots, n, rows, nv), bf16),
            pltpu.VMEM((slots, n * rows, nv), bf16),
            pltpu.VMEM((pairs, roots, nv, width), bf16),
            pltpu.VMEM((pairs, nv, roots * width), bf16),
            pltpu.VMEM((pairs, roots, width, width), bf16),
            pltpu.VMEM((pairs, roots, width, width), jnp.float32),
            pltpu.VMEM((m, pairs, roots, strip, width), bf16),
            pltpu.VMEM((m - 1, pairs, roots, strip, width), bf16),
            pltpu.VMEM((pairs, roots, strip, width), bf16),
            pltpu.SMEM((slots,), jnp.int32),
            pltpu.SMEM((pairs,), jnp.int32),
            pltpu.SMEM((pairs,), jnp.int32),
            pltpu.SMEM((1, 128), jnp.int32),
            pltpu.SMEM((chips, 1, 128), jnp.int32),
            dma((3,)),
            dma,
            dma((slots,)),
            dma((2,)),
            dma,
            dma((pairs - complete_after(slots, pairs)[-2] + 1,)),
            pltpu.SemaphoreType.REGULAR,
            pltpu.SemaphoreType.REGULAR,
        ],
        compiler_params=pltpu.CompilerParams(
            collective_id=0, has_side_effects=True, vmem_limit_bytes=60 * 2**20
        ),
    )(domain, pair_slots.T, ranks.T, panels, transforms, trial)


def solution(mesh):
    return jax.shard_map(
        functools.partial(per_device, mesh.shape["pairs"], mesh.shape["aux"]),
        mesh=mesh,
        in_specs=(
            P(None, ("pairs", "aux"), None),
            P(),
            P("pairs", None),
            P("pairs", None),
            P("pairs", None, None, None),
            P("pairs", None, None, None),
        ),
        out_specs=P("pairs", None, "aux", None),
        check_vma=False,
    )
```

```python
import functools

import jax
import jax.numpy as jnp
from jax import lax
from jax.experimental import pallas as pl
from jax.experimental.pallas import tpu as pltpu
from jax.sharding import PartitionSpec as P

MESH = pl.DeviceIdType.MESH
CORES = 2
BATCH = 4
FIXED = 2


def peer_of(me, offset, count):
    if count & (count - 1):
        return lax.rem(me + offset, count)
    peer = me
    bit = 1
    while bit < count:
        if offset & bit:
            peer = peer + bit * (1 - 2 * lax.rem(me // bit, 2))
        bit *= 2
    return peer


def complete_after(slots, pairs, fixed):
    sure = pairs
    counts = [pairs]
    for left in range(slots, 1, -1):
        sure -= min(sure, 2 * sure // (left - fixed)) if left > fixed else sure
        counts.insert(0, sure)
    return counts


def elimination(slots_ref, slots, pairs, fixed):
    bits = (pairs + 1).bit_length()
    left = [slots_ref[0, pair] for pair in range(pairs)]
    right = [slots_ref[1, pair] for pair in range(pairs)]
    fields = 31 // bits
    words = -(-slots // fields)

    def mark(slot, word):
        low = word * fields
        shift = slot - low
        inside = (shift >= 0) & (shift < fields)
        return jnp.where(inside, jnp.left_shift(1, jnp.where(inside, shift, 0) * bits), 0)

    marks = [[mark(left[p], w) | mark(right[p], w) for w in range(words)] for p in range(pairs)]
    alive = [jnp.int32(1)] * pairs
    rank = [jnp.int32(0)] * pairs
    place = [jnp.int32(0)] * slots
    taken = [jnp.int32(0)] * slots
    for spot in range(slots - 1, -1, -1):
        totals = [sum(alive[p] * marks[p][w] for p in range(pairs)) for w in range(words)]
        best, pick = None, None
        for slot in range(slots):
            count = (totals[slot // fields] >> (bits * (slot % fields))) & (2**bits - 1)
            count = count + (taken[slot] * (slots + 1) + jnp.maximum(fixed - slot, 0)) * 2**bits
            if best is None:
                best, pick = count, jnp.int32(slot)
            else:
                less = count < best
                best = jnp.where(less, count, best)
                pick = jnp.where(less, slot, pick)
        for slot in range(slots):
            hit = pick == slot
            place[slot] = jnp.where(hit, spot, place[slot])
            taken[slot] = jnp.where(hit, 1, taken[slot])
        gone = []
        for p in range(pairs):
            touch = (left[p] == pick) | (right[p] == pick)
            gone.append(jnp.where(touch, alive[p], 0))
            alive[p] = alive[p] - gone[p]
        at = sum(alive)
        for p in range(pairs):
            rank[p] = jnp.where(gone[p] == 1, at, rank[p])
            at = at + gone[p]
    return place, rank


def fused_kernel(
    n, m, domain_ref, slots_ref, ranks_ref, panels_ref, d_ref, c_ref, out_ref,
    panels, outgoing, recv, block, turned, d_raw, d_mask, d_turned, c_raw, c_pair, acc, send_buf, landed, total,
    place_ref, rank_ref, perm_ref, mine_order, landed_orders, orders,
    local_sem, send_sem, recv_sem, order_sem, part_send, part_recv, from_below, from_above,
):
    me = lax.axis_index("pairs")
    mine = lax.axis_index("aux")
    core = lax.rem(me, CORES)
    chip = me // CORES
    chips = n // CORES
    pairs, roots, nv, width = d_ref.shape
    slots = domain_ref.shape[1]
    rows = panels_ref.shape[1]
    strip = width // m
    early = complete_after(slots, pairs, 0)[-2] - 1

    def device(k, dest):
        return peer_of(chip, k, chips) * CORES + dest

    barrier = pltpu.get_barrier_semaphore()
    for k in range(chips):
        for dest in range(CORES):
            if k:
                pl.semaphore_signal(barrier, inc=1, device_id=(device(k, dest), mine), device_id_type=MESH)
    pl.semaphore_signal(barrier, inc=1, device_id=(chip * CORES + 1 - core, mine), device_id_type=MESH)

    @pl.when(mine > 0)
    def _():
        pl.semaphore_signal(barrier, inc=1, device_id=(me, mine - 1), device_id_type=MESH)

    @pl.when(mine < m - 1)
    def _():
        pl.semaphore_signal(barrier, inc=1, device_id=(me, mine + 1), device_id_type=MESH)

    panels_copy = pltpu.make_async_copy(panels_ref, panels, local_sem.at[0])
    panels_copy.start()
    d_copy = pltpu.make_async_copy(d_ref, d_raw, local_sem.at[1])
    d_copy.start()
    c_copy = pltpu.make_async_copy(c_ref, c_raw, local_sem.at[2])
    c_copy.start()

    place, rank = elimination(slots_ref, slots, pairs, jnp.where(core == 0, FIXED, 0))
    for slot in range(slots):
        place_ref[slot] = place[slot]
    for pair in range(pairs):
        rank_ref[pair] = rank[pair]
    lanes = lax.broadcasted_iota(jnp.int32, (1, 128), 1)
    own_order = []
    for spot in range(slots):
        chosen = sum(jnp.where(place[slot] == spot, slot, 0) for slot in range(slots))
        own_order.append(chosen)
    line = jnp.zeros((1, 128), jnp.int32)
    for spot in range(slots):
        line = jnp.where(lanes == spot, own_order[spot], line)
    mine_order[...] = line
    for q in range(pairs):
        perm_ref[q] = sum(jnp.where(rank[pair] == q, pair, 0) for pair in range(pairs))

    beside = jnp.where(mine > 0, 1, 0) + jnp.where(mine < m - 1, 1, 0)
    pl.semaphore_wait(barrier, n - 1 + beside)

    def order_copy(peer):
        return pltpu.make_async_remote_copy(
            src_ref=mine_order,
            dst_ref=landed_orders.at[me],
            send_sem=order_sem.at[0],
            recv_sem=order_sem.at[1],
            device_id=(peer, mine),
            device_id_type=MESH,
        )

    for k in range(1, chips):
        for dest in range(CORES):
            order_copy(device(k, dest)).start()
    order_copy(chip * CORES + 1 - core).start()

    panels_copy.wait()

    def panel_copy(k, dest, spot):
        return pltpu.make_async_remote_copy(
            src_ref=outgoing.at[dest, k, spot],
            dst_ref=recv.at[spot, k * CORES + core],
            send_sem=send_sem,
            recv_sem=recv_sem.at[spot],
            device_id=(device(k, dest), mine),
            device_id_type=MESH,
        )

    def gather(dest, k, spot, ordered=True):
        peer = device(k, dest)
        slot = orders[peer, 0, jnp.minimum(spot, slots - 1)] if ordered else spot
        outgoing[dest, k, spot] = panels[domain_ref[peer, slot]]

    def send_near(dest, spots, ordered=True):
        for spot in spots:
            gather(dest, 0, spot, ordered)

        @pl.when(core != dest)
        def _():
            for spot in spots:
                panel_copy(0, dest, spot).start()

        @pl.when(core == dest)
        def _():
            for spot in spots:
                recv[spot, dest] = outgoing[dest, 0, spot]

    def send_far(dest, spots, ordered=True):
        waiting = None
        for spot in spots:
            for k in range(1, chips):
                gather(dest, k, spot, ordered)
                if waiting is not None:
                    waiting.start()
                waiting = panel_copy(k, dest, spot)
        waiting.start()

    def send_led(dest):
        def spot_of(k, turn):
            ahead = peer_of(chip, k, chips) == 0
            spot = jnp.where(ahead, turn + 1, jnp.where(turn < 0, slots, turn))
            return spot, spot < slots

        def start(k, turn):
            spot, real = spot_of(k, turn)

            @pl.when(real)
            def _():
                panel_copy(k, dest, jnp.minimum(spot, slots - 1)).start()

        rounds = [(k, turn) for turn in range(-1, slots) for k in range(1, chips)]
        for index, (k, turn) in enumerate(rounds):
            gather(dest, k, spot_of(k, turn)[0])
            if index:
                start(*rounds[index - 1])
        start(*rounds[-1])

    def orders_done(sem):
        whole = landed_orders.at[pl.ds(0, n - 1)]
        pltpu.make_async_copy(whole, whole, order_sem.at[sem]).wait()

    send_far(0, range(FIXED), ordered=False)
    send_near(0, range(FIXED), ordered=False)
    landed_orders[me] = mine_order[...]
    orders_done(1)
    orders_copy = pltpu.make_async_copy(landed_orders, orders, local_sem.at[3])
    orders_copy.start()
    orders_copy.wait()
    send_far(0, range(FIXED, slots))
    for dest in range(1, CORES):
        send_led(dest)
        send_near(dest, range(slots))
    send_near(0, range(FIXED, slots))

    for far in range(2, m):

        @pl.when((mine >= far - 1) & (mine < m - 1))
        def _():
            pl.semaphore_signal(from_below, inc=1, device_id=(me, mine + 1), device_id_type=MESH)

        @pl.when((mine <= m - far) & (mine > 0))
        def _():
            pl.semaphore_signal(from_above, inc=1, device_id=(me, mine - 1), device_id_type=MESH)

        @pl.when(mine >= far)
        def _():
            pl.semaphore_wait(from_below, 1)

        @pl.when(mine < m - far)
        def _():
            pl.semaphore_wait(from_above, 1)

    columns = lax.broadcasted_iota(jnp.int32, (1, width), 1)
    row_ids = lax.broadcasted_iota(jnp.int32, (width, 1), 0)
    d_copy.wait()
    c_copy.wait()

    def mask_pair(pair, carry):
        for root in range(roots):
            limit = ranks_ref[root, pair]
            kept = jnp.where(columns < limit, d_raw[pair, root], jnp.zeros((), d_raw.dtype))
            d_mask[pair, :, root * width:(root + 1) * width] = kept
            d_turned[pair, root * width:(root + 1) * width] = kept.T
            keep = (columns < limit) & (row_ids < limit)
            kept = jnp.where(keep, c_raw[pair, root], jnp.zeros((), c_raw.dtype))
            c_pair[pair, root, :, :width] = kept
            c_pair[pair, root, :, width:] = kept.T
        return carry

    lax.fori_loop(0, pairs, mask_pair, 0)

    def part_copy(q, owner):
        return pltpu.make_async_remote_copy(
            src_ref=send_buf.at[owner, q],
            dst_ref=landed.at[mine, q],
            send_sem=part_send,
            recv_sem=part_recv.at[max(q - early, 0)],
            device_id=(me, owner),
            device_id_type=MESH,
        )

    def split(value):
        high = value.astype(jnp.bfloat16)
        return high, (value - high.astype(jnp.float32)).astype(jnp.bfloat16)

    def dot(left, right):
        return jnp.dot(left, right, preferred_element_type=jnp.float32)

    def compute(first, count):
        qs = [first + index for index in range(count)]
        which = [perm_ref[q] for q in qs]
        grams = [
            dot(turned[place_ref[slots_ref[0, pair]]], block[place_ref[slots_ref[1, pair]]]) for pair in which
        ]
        halves = []
        for gram, pair in zip(grams, which):
            both = dot(jnp.concatenate(split(gram), axis=0), d_mask[pair])
            halves.append(both[:nv] + both[nv:])
        wholes = []
        for half, pair in zip(halves, which):
            high, low = split(half)
            wholes.append(dot(d_turned[pair], high) + dot(d_turned[pair], low))
        kmats = [
            [whole[root * width:(root + 1) * width, root * width:(root + 1) * width] for root in range(roots)]
            for whole in wholes
        ]
        sides = [
            [dot(kmat[root].astype(jnp.bfloat16), c_pair[pair, root]) for root in range(roots)]
            for kmat, pair in zip(kmats, which)
        ]
        for q, kmat, side in zip(qs, kmats, sides):
            for root in range(roots):
                sigma = kmat[root] + side[root][:, :width] + side[root][:, width:].T
                acc[q, root] = sigma
                for owner in range(m):
                    send_buf[owner, q, root] = sigma[owner * strip:(owner + 1) * strip].astype(jnp.bfloat16)
        for owner in range(m):

            @pl.when(mine != owner)
            def _():
                for q in qs:
                    part_copy(q, owner).start()

    def take(spot):
        others = recv.at[spot, pl.ds(0, n - 1)]
        pltpu.make_async_copy(others, others, recv_sem.at[spot]).wait()
        whole = recv[spot].reshape(n * rows, nv)
        block[spot] = whole
        turned[spot] = whole.T

    def run(counts, spot):
        done = counts[spot - 1] if spot else 0
        while done < counts[spot]:
            step = min(BATCH, counts[spot] - done)
            compute(done, step)
            done += step

    for spot in range(slots):
        take(spot)

        @pl.when(core == 0)
        def _():
            run(complete_after(slots, pairs, FIXED), spot)

        @pl.when(core != 0)
        def _():
            run(complete_after(slots, pairs, 0), spot)

    gone = outgoing.at[:, pl.ds(1, chips - 1), pl.ds(0, slots)]
    pltpu.make_async_copy(gone, gone, send_sem).wait()
    gone = outgoing.at[0, 0, pl.ds(0, slots)]
    pltpu.make_async_copy(gone, gone, send_sem).wait()

    orders_done(0)

    def sum_of(q):
        value = acc[q, :, pl.ds(pl.multiple_of(mine * strip, strip), strip), :]
        for offset in range(1, m):
            value = value + landed[lax.rem(mine + offset, m), q].astype(jnp.float32)
        total[q] = value.astype(total.dtype)

    lots = landed.at[pl.ds(0, m - 1), pl.ds(0, early + 1)]
    pltpu.make_async_copy(lots, lots, part_recv.at[0]).wait()
    for q in range(early + 1):
        sum_of(q)
    for q in range(early + 1, pairs):
        lot = landed.at[pl.ds(0, m - 1), q]
        pltpu.make_async_copy(lot, lot, part_recv.at[q - early]).wait()
        sum_of(q)
    for pair in range(pairs):
        out_ref[pair] = total[rank_ref[pair]]
    sent = send_buf.at[pl.ds(0, m - 1)]
    pltpu.make_async_copy(sent, sent, part_send).wait()


def per_device(n, m, panels, domain, pair_slots, ranks, transforms, trial):
    pairs, roots, nv, width = transforms.shape
    slots = domain.shape[1]
    rows = panels.shape[1]
    chips = n // CORES
    strip = width // m
    bf16 = jnp.bfloat16
    smem = pl.BlockSpec(memory_space=pltpu.SMEM)
    hbm = pl.BlockSpec(memory_space=pltpu.HBM)
    dma = pltpu.SemaphoreType.DMA
    return pl.pallas_call(
        functools.partial(fused_kernel, n, m),
        in_specs=[smem, smem, smem, hbm, hbm, hbm],
        out_specs=pl.BlockSpec(memory_space=pltpu.VMEM),
        out_shape=pltpu.VMEM((pairs, roots, strip, width), bf16),
        scratch_shapes=[
            pltpu.VMEM(panels.shape, bf16),
            pltpu.VMEM((CORES, chips, slots + 1, rows, nv), bf16),
            pltpu.VMEM((slots, n, rows, nv), bf16),
            pltpu.VMEM((slots, n * rows, nv), bf16),
            pltpu.VMEM((slots, nv, n * rows), bf16),
            pltpu.VMEM((pairs, roots, nv, width), bf16),
            pltpu.VMEM((pairs, nv, roots * width), bf16),
            pltpu.VMEM((pairs, roots * width, nv), bf16),
            pltpu.VMEM((pairs, roots, width, width), bf16),
            pltpu.VMEM((pairs, roots, width, 2 * width), bf16),
            pltpu.VMEM((pairs, roots, width, width), jnp.float32),
            pltpu.VMEM((m, pairs, roots, strip, width), bf16),
            pltpu.VMEM((m, pairs, roots, strip, width), bf16),
            pltpu.VMEM((pairs, roots, strip, width), bf16),
            pltpu.SMEM((slots,), jnp.int32),
            pltpu.SMEM((pairs,), jnp.int32),
            pltpu.SMEM((pairs,), jnp.int32),
            pltpu.VMEM((1, 128), jnp.int32),
            pltpu.VMEM((n, 1, 128), jnp.int32),
            pltpu.SMEM((n, 1, 128), jnp.int32),
            dma((4,)),
            dma,
            dma((slots,)),
            dma((2,)),
            dma,
            dma((pairs - complete_after(slots, pairs, 0)[-2] + 1,)),
            pltpu.SemaphoreType.REGULAR,
            pltpu.SemaphoreType.REGULAR,
        ],
        compiler_params=pltpu.CompilerParams(
            collective_id=0, has_side_effects=True, vmem_limit_bytes=60 * 2**20
        ),
    )(domain, pair_slots.T, ranks.T, panels, transforms, trial)


def solution(mesh):
    return jax.shard_map(
        functools.partial(per_device, mesh.shape["pairs"], mesh.shape["aux"]),
        mesh=mesh,
        in_specs=(
            P(None, ("pairs", "aux"), None),
            P(),
            P("pairs", None),
            P("pairs", None),
            P("pairs", None, None, None),
            P("pairs", None, None, None),
        ),
        out_specs=P("pairs", None, "aux", None),
        check_vma=False,
    )
```

```python
import functools

import jax
import jax.numpy as jnp
from jax import lax
from jax.experimental import pallas as pl
from jax.experimental.pallas import tpu as pltpu
from jax.sharding import PartitionSpec as P

MESH = pl.DeviceIdType.MESH
CORES = 2
BATCH = 4
LATE = 4
FIXED = 2


def peer_of(me, offset, count):
    if count & (count - 1):
        return lax.rem(me + offset, count)
    peer = me
    bit = 1
    while bit < count:
        if offset & bit:
            peer = peer + bit * (1 - 2 * lax.rem(me // bit, 2))
        bit *= 2
    return peer


def complete_after(slots, pairs, fixed):
    sure = pairs
    counts = [pairs]
    for left in range(slots, 1, -1):
        sure -= min(sure, 2 * sure // (left - fixed)) if left > fixed else sure
        counts.insert(0, sure)
    return counts


def elimination(slots_ref, slots, pairs, fixed):
    bits = (pairs + 1).bit_length()
    left = [slots_ref[0, pair] for pair in range(pairs)]
    right = [slots_ref[1, pair] for pair in range(pairs)]
    fields = 31 // bits
    words = -(-slots // fields)

    def mark(slot, word):
        low = word * fields
        shift = slot - low
        inside = (shift >= 0) & (shift < fields)
        return jnp.where(inside, jnp.left_shift(1, jnp.where(inside, shift, 0) * bits), 0)

    marks = [[mark(left[p], w) | mark(right[p], w) for w in range(words)] for p in range(pairs)]
    alive = [jnp.int32(1)] * pairs
    rank = [jnp.int32(0)] * pairs
    place = [jnp.int32(0)] * slots
    taken = [jnp.int32(0)] * slots
    for spot in range(slots - 1, -1, -1):
        totals = [sum(alive[p] * marks[p][w] for p in range(pairs)) for w in range(words)]
        best, pick = None, None
        for slot in range(slots):
            count = (totals[slot // fields] >> (bits * (slot % fields))) & (2**bits - 1)
            count = count + (taken[slot] * (slots + 1) + jnp.maximum(fixed - slot, 0)) * 2**bits
            if best is None:
                best, pick = count, jnp.int32(slot)
            else:
                less = count < best
                best = jnp.where(less, count, best)
                pick = jnp.where(less, slot, pick)
        for slot in range(slots):
            hit = pick == slot
            place[slot] = jnp.where(hit, spot, place[slot])
            taken[slot] = jnp.where(hit, 1, taken[slot])
        gone = []
        for p in range(pairs):
            touch = (left[p] == pick) | (right[p] == pick)
            gone.append(jnp.where(touch, alive[p], 0))
            alive[p] = alive[p] - gone[p]
        at = sum(alive)
        for p in range(pairs):
            rank[p] = jnp.where(gone[p] == 1, at, rank[p])
            at = at + gone[p]
    return place, rank


def fused_kernel(
    n, m, domain_in, slots_in, ranks_in, panels_ref, d_ref, c_ref, out_ref,
    domain_ref, slots_ref, ranks_ref,
    panels, outgoing, recv, block, turned, d_raw, d_mask, d_turned, c_raw, c_pair, acc, send_buf, landed, total,
    place_ref, rank_ref, perm_ref, mine_order, landed_orders, orders,
    local_sem, send_sem, recv_sem, order_sem, part_send, part_recv, from_below, from_above,
):
    me = lax.axis_index("pairs")
    mine = lax.axis_index("aux")
    core = lax.rem(me, CORES)
    chip = me // CORES
    chips = n // CORES
    pairs, roots, nv, width = d_ref.shape
    slots = domain_in.shape[1]
    rows = panels_ref.shape[1]
    strip = width // m
    early = complete_after(slots, pairs, 0)[-2]

    def group_of(q):
        return 0 if q < early else 1 + (q - early) // LATE


    def device(k, dest):
        return peer_of(chip, k, chips) * CORES + dest

    barrier = pltpu.get_barrier_semaphore()
    for k in range(chips):
        for dest in range(CORES):
            if k:
                pl.semaphore_signal(barrier, inc=1, device_id=(device(k, dest), mine), device_id_type=MESH)
    pl.semaphore_signal(barrier, inc=1, device_id=(chip * CORES + 1 - core, mine), device_id_type=MESH)

    @pl.when(mine > 0)
    def _():
        pl.semaphore_signal(barrier, inc=1, device_id=(me, mine - 1), device_id_type=MESH)

    @pl.when(mine < m - 1)
    def _():
        pl.semaphore_signal(barrier, inc=1, device_id=(me, mine + 1), device_id_type=MESH)

    small = [
        pltpu.make_async_copy(source, target, local_sem.at[4 + index])
        for index, (source, target) in enumerate(
            [(slots_in, slots_ref), (domain_in, domain_ref), (ranks_in, ranks_ref)]
        )
    ]
    for copy in small:
        copy.start()
    panels_copy = pltpu.make_async_copy(panels_ref, panels, local_sem.at[0])
    panels_copy.start()
    d_copy = pltpu.make_async_copy(d_ref, d_raw, local_sem.at[1])
    d_copy.start()
    c_copy = pltpu.make_async_copy(c_ref, c_raw, local_sem.at[2])
    c_copy.start()

    for copy in small:
        copy.wait()
    place, rank = elimination(slots_ref, slots, pairs, jnp.where(core == 0, FIXED, 0))
    for slot in range(slots):
        place_ref[slot] = place[slot]
    for pair in range(pairs):
        rank_ref[pair] = rank[pair]
    lanes = lax.broadcasted_iota(jnp.int32, (1, 128), 1)
    own_order = []
    for spot in range(slots):
        chosen = sum(jnp.where(place[slot] == spot, slot, 0) for slot in range(slots))
        own_order.append(chosen)
    line = jnp.zeros((1, 128), jnp.int32)
    for spot in range(slots):
        line = jnp.where(lanes == spot, own_order[spot], line)
    mine_order[...] = line
    for q in range(pairs):
        perm_ref[q] = sum(jnp.where(rank[pair] == q, pair, 0) for pair in range(pairs))

    beside = jnp.where(mine > 0, 1, 0) + jnp.where(mine < m - 1, 1, 0)
    pl.semaphore_wait(barrier, n - 1 + beside)

    def order_copy(peer):
        return pltpu.make_async_remote_copy(
            src_ref=mine_order,
            dst_ref=landed_orders.at[me],
            send_sem=order_sem.at[0],
            recv_sem=order_sem.at[1],
            device_id=(peer, mine),
            device_id_type=MESH,
        )

    for k in range(1, chips):
        for dest in range(CORES):
            order_copy(device(k, dest)).start()
    order_copy(chip * CORES + 1 - core).start()

    panels_copy.wait()

    def panel_copy(k, dest, spot):
        return pltpu.make_async_remote_copy(
            src_ref=outgoing.at[dest, k, spot],
            dst_ref=recv.at[spot, k * CORES + core],
            send_sem=send_sem,
            recv_sem=recv_sem.at[spot],
            device_id=(device(k, dest), mine),
            device_id_type=MESH,
        )

    def gather(dest, k, spot, ordered=True):
        peer = device(k, dest)
        slot = orders[peer, 0, jnp.minimum(spot, slots - 1)] if ordered else spot
        outgoing[dest, k, spot] = panels[domain_ref[peer, slot]]

    def send_near(dest, spots, ordered=True):
        for spot in spots:
            gather(dest, 0, spot, ordered)

        @pl.when(core != dest)
        def _():
            for spot in spots:
                panel_copy(0, dest, spot).start()

        @pl.when(core == dest)
        def _():
            for spot in spots:
                recv[spot, dest] = outgoing[dest, 0, spot]

    def send_far(dest, spots, ordered=True):
        waiting = None
        for spot in spots:
            for k in range(1, chips):
                gather(dest, k, spot, ordered)
                if waiting is not None:
                    waiting.start()
                waiting = panel_copy(k, dest, spot)
        waiting.start()

    def send_led(dest):
        def spot_of(k, turn):
            ahead = peer_of(chip, k, chips) == 0
            spot = jnp.where(ahead, turn + 1, jnp.where(turn < 0, slots, turn))
            return spot, spot < slots

        def start(k, turn):
            spot, real = spot_of(k, turn)

            @pl.when(real)
            def _():
                panel_copy(k, dest, jnp.minimum(spot, slots - 1)).start()

        rounds = [(k, turn) for turn in range(-1, slots) for k in range(1, chips)]
        for index, (k, turn) in enumerate(rounds):
            gather(dest, k, spot_of(k, turn)[0])
            if index:
                start(*rounds[index - 1])
        start(*rounds[-1])

    def orders_done(sem):
        whole = landed_orders.at[pl.ds(0, n - 1)]
        pltpu.make_async_copy(whole, whole, order_sem.at[sem]).wait()

    send_far(0, range(FIXED), ordered=False)
    send_near(0, range(FIXED), ordered=False)
    landed_orders[me] = mine_order[...]
    orders_done(1)
    orders_copy = pltpu.make_async_copy(landed_orders, orders, local_sem.at[3])
    orders_copy.start()
    orders_copy.wait()
    send_far(0, range(FIXED, slots))
    for dest in range(1, CORES):
        send_led(dest)
        send_near(dest, range(slots))
    send_near(0, range(FIXED, slots))

    for far in range(2, m):

        @pl.when((mine >= far - 1) & (mine < m - 1))
        def _():
            pl.semaphore_signal(from_below, inc=1, device_id=(me, mine + 1), device_id_type=MESH)

        @pl.when((mine <= m - far) & (mine > 0))
        def _():
            pl.semaphore_signal(from_above, inc=1, device_id=(me, mine - 1), device_id_type=MESH)

        @pl.when(mine >= far)
        def _():
            pl.semaphore_wait(from_below, 1)

        @pl.when(mine < m - far)
        def _():
            pl.semaphore_wait(from_above, 1)

    columns = lax.broadcasted_iota(jnp.int32, (1, width), 1)
    row_ids = lax.broadcasted_iota(jnp.int32, (width, 1), 0)
    d_copy.wait()
    c_copy.wait()

    def mask_pair(pair, carry):
        for root in range(roots):
            limit = ranks_ref[root, pair]
            kept = jnp.where(columns < limit, d_raw[pair, root], jnp.zeros((), d_raw.dtype))
            d_mask[pair, :, root * width:(root + 1) * width] = kept
            d_turned[pair, root * width:(root + 1) * width] = kept.T
            keep = (columns < limit) & (row_ids < limit)
            kept = jnp.where(keep, c_raw[pair, root], jnp.zeros((), c_raw.dtype))
            c_pair[pair, root, :, :width] = kept
            c_pair[pair, root, :, width:] = kept.T
        return carry

    lax.fori_loop(0, pairs, mask_pair, 0)

    def part_copy(q, owner):
        return pltpu.make_async_remote_copy(
            src_ref=send_buf.at[owner, q],
            dst_ref=landed.at[mine, q],
            send_sem=part_send,
            recv_sem=part_recv.at[group_of(q)],
            device_id=(me, owner),
            device_id_type=MESH,
        )

    def split(value):
        high = value.astype(jnp.bfloat16)
        return high, (value - high.astype(jnp.float32)).astype(jnp.bfloat16)

    def dot(left, right):
        return jnp.dot(left, right, preferred_element_type=jnp.float32)

    def compute(first, count):
        qs = [first + index for index in range(count)]
        which = [perm_ref[q] for q in qs]
        grams = [
            dot(turned[place_ref[slots_ref[0, pair]]], block[place_ref[slots_ref[1, pair]]]) for pair in which
        ]
        halves = []
        for gram, pair in zip(grams, which):
            both = dot(jnp.concatenate(split(gram), axis=0), d_mask[pair])
            halves.append(both[:nv] + both[nv:])
        wholes = []
        for half, pair in zip(halves, which):
            high, low = split(half)
            wholes.append(dot(d_turned[pair], high) + dot(d_turned[pair], low))
        kmats = [
            [whole[root * width:(root + 1) * width, root * width:(root + 1) * width] for root in range(roots)]
            for whole in wholes
        ]
        sides = [
            [dot(kmat[root].astype(jnp.bfloat16), c_pair[pair, root]) for root in range(roots)]
            for kmat, pair in zip(kmats, which)
        ]
        for q, kmat, side in zip(qs, kmats, sides):
            for root in range(roots):
                sigma = kmat[root] + side[root][:, :width] + side[root][:, width:].T
                acc[q, root] = sigma
                for owner in range(m):
                    send_buf[owner, q, root] = sigma[owner * strip:(owner + 1) * strip].astype(jnp.bfloat16)
        for owner in range(m):

            @pl.when(mine != owner)
            def _():
                for q in qs:
                    part_copy(q, owner).start()

    def take(spot):
        others = recv.at[spot, pl.ds(0, n - 1)]
        pltpu.make_async_copy(others, others, recv_sem.at[spot]).wait()
        whole = recv[spot].reshape(n * rows, nv)
        block[spot] = whole
        turned[spot] = whole.T

    def run(counts, spot):
        done = counts[spot - 1] if spot else 0
        while done < counts[spot]:
            limit = min(BATCH, early - done) if done < early else LATE - (done - early) % LATE
            step = min(limit, counts[spot] - done)
            compute(done, step)
            done += step

    for spot in range(slots):
        take(spot)

        @pl.when(core == 0)
        def _():
            run(complete_after(slots, pairs, FIXED), spot)

        @pl.when(core != 0)
        def _():
            run(complete_after(slots, pairs, 0), spot)

    gone = outgoing.at[:, pl.ds(1, chips - 1), pl.ds(0, slots)]
    pltpu.make_async_copy(gone, gone, send_sem).wait()
    gone = outgoing.at[0, 0, pl.ds(0, slots)]
    pltpu.make_async_copy(gone, gone, send_sem).wait()

    orders_done(0)

    edges = [0, *range(early, pairs, LATE), pairs]
    for group, (low, high) in enumerate(zip(edges, edges[1:])):
        part = pl.ds(low, high - low)
        lot = landed.at[pl.ds(0, m - 1), part]
        pltpu.make_async_copy(lot, lot, part_recv.at[group]).wait()
        value = acc[part, :, pl.ds(pl.multiple_of(mine * strip, strip), strip), :]
        for offset in range(1, m):
            value = value + landed[lax.rem(mine + offset, m), part].astype(jnp.float32)
        total[part] = value.astype(total.dtype)
    for pair in range(pairs):
        out_ref[pair] = total[rank_ref[pair]]
    sent = send_buf.at[pl.ds(0, m - 1)]
    pltpu.make_async_copy(sent, sent, part_send).wait()


def per_device(n, m, panels, domain, pair_slots, ranks, transforms, trial):
    pairs, roots, nv, width = transforms.shape
    slots = domain.shape[1]
    rows = panels.shape[1]
    chips = n // CORES
    strip = width // m
    bf16 = jnp.bfloat16
    hbm = pl.BlockSpec(memory_space=pltpu.HBM)
    dma = pltpu.SemaphoreType.DMA
    return pl.pallas_call(
        functools.partial(fused_kernel, n, m),
        in_specs=[hbm] * 6,
        out_specs=pl.BlockSpec(memory_space=pltpu.VMEM),
        out_shape=pltpu.VMEM((pairs, roots, strip, width), bf16),
        scratch_shapes=[
            pltpu.SMEM(domain.shape, jnp.int32),
            pltpu.SMEM(pair_slots.shape[::-1], jnp.int32),
            pltpu.SMEM(ranks.shape[::-1], jnp.int32),
            pltpu.VMEM(panels.shape, bf16),
            pltpu.VMEM((CORES, chips, slots + 1, rows, nv), bf16),
            pltpu.VMEM((slots, n, rows, nv), bf16),
            pltpu.VMEM((slots, n * rows, nv), bf16),
            pltpu.VMEM((slots, nv, n * rows), bf16),
            pltpu.VMEM((pairs, roots, nv, width), bf16),
            pltpu.VMEM((pairs, nv, roots * width), bf16),
            pltpu.VMEM((pairs, roots * width, nv), bf16),
            pltpu.VMEM((pairs, roots, width, width), bf16),
            pltpu.VMEM((pairs, roots, width, 2 * width), bf16),
            pltpu.VMEM((pairs, roots, width, width), jnp.float32),
            pltpu.VMEM((m, pairs, roots, strip, width), bf16),
            pltpu.VMEM((m, pairs, roots, strip, width), bf16),
            pltpu.VMEM((pairs, roots, strip, width), bf16),
            pltpu.SMEM((slots,), jnp.int32),
            pltpu.SMEM((pairs,), jnp.int32),
            pltpu.SMEM((pairs,), jnp.int32),
            pltpu.VMEM((1, 128), jnp.int32),
            pltpu.VMEM((n, 1, 128), jnp.int32),
            pltpu.SMEM((n, 1, 128), jnp.int32),
            dma((7,)),
            dma,
            dma((slots,)),
            dma((2,)),
            dma,
            dma((1 - (complete_after(slots, pairs, 0)[-2] - pairs) // LATE,)),
            pltpu.SemaphoreType.REGULAR,
            pltpu.SemaphoreType.REGULAR,
        ],
        compiler_params=pltpu.CompilerParams(
            collective_id=0, has_side_effects=True, vmem_limit_bytes=60 * 2**20
        ),
    )(domain, pair_slots.T, ranks.T, panels, transforms, trial)


def solution(mesh):
    return jax.shard_map(
        functools.partial(per_device, mesh.shape["pairs"], mesh.shape["aux"]),
        mesh=mesh,
        in_specs=(
            P(None, ("pairs", "aux"), None),
            P(),
            P("pairs", None),
            P("pairs", None),
            P("pairs", None, None, None),
            P("pairs", None, None, None),
        ),
        out_specs=P("pairs", None, "aux", None),
        check_vma=False,
    )
```

```python
import functools

import jax
import jax.numpy as jnp
from jax import lax
from jax.experimental import pallas as pl
from jax.experimental.pallas import tpu as pltpu
from jax.sharding import PartitionSpec as P

MESH = pl.DeviceIdType.MESH
CORES = 2
BATCH = 4
LATE = 4
FIXED = 2


def peer_of(me, offset, count):
    if count & (count - 1):
        return lax.rem(me + offset, count)
    peer = me
    bit = 1
    while bit < count:
        if offset & bit:
            peer = peer + bit * (1 - 2 * lax.rem(me // bit, 2))
        bit *= 2
    return peer


def complete_after(slots, pairs, fixed):
    sure = pairs
    counts = [pairs]
    for left in range(slots, 1, -1):
        sure -= min(sure, 2 * sure // (left - fixed)) if left > fixed else sure
        counts.insert(0, sure)
    return counts


def elimination(slots_ref, slots, pairs, fixed):
    bits = (pairs + 1).bit_length()
    left = [slots_ref[0, pair] for pair in range(pairs)]
    right = [slots_ref[1, pair] for pair in range(pairs)]
    fields = 31 // bits
    words = -(-slots // fields)

    def mark(slot, word):
        low = word * fields
        shift = slot - low
        inside = (shift >= 0) & (shift < fields)
        return jnp.where(inside, jnp.left_shift(1, jnp.where(inside, shift, 0) * bits), 0)

    marks = [[mark(left[p], w) | mark(right[p], w) for w in range(words)] for p in range(pairs)]
    alive = [jnp.int32(1)] * pairs
    rank = [jnp.int32(0)] * pairs
    place = [jnp.int32(0)] * slots
    taken = [jnp.int32(0)] * slots
    for spot in range(slots - 1, -1, -1):
        totals = [sum(alive[p] * marks[p][w] for p in range(pairs)) for w in range(words)]
        best, pick = None, None
        for slot in range(slots):
            count = (totals[slot // fields] >> (bits * (slot % fields))) & (2**bits - 1)
            count = count + (taken[slot] * (slots + 1) + jnp.maximum(fixed - slot, 0)) * 2**bits
            if best is None:
                best, pick = count, jnp.int32(slot)
            else:
                less = count < best
                best = jnp.where(less, count, best)
                pick = jnp.where(less, slot, pick)
        for slot in range(slots):
            hit = pick == slot
            place[slot] = jnp.where(hit, spot, place[slot])
            taken[slot] = jnp.where(hit, 1, taken[slot])
        gone = []
        for p in range(pairs):
            touch = (left[p] == pick) | (right[p] == pick)
            gone.append(jnp.where(touch, alive[p], 0))
            alive[p] = alive[p] - gone[p]
        at = sum(alive)
        for p in range(pairs):
            rank[p] = jnp.where(gone[p] == 1, at, rank[p])
            at = at + gone[p]
    return place, rank


def fused_kernel(
    n, m, domain_in, slots_in, ranks_in, panels_ref, d_ref, c_ref, out_ref,
    domain_ref, slots_ref, ranks_ref,
    panels, outgoing, recv, block, turned, d_raw, d_mask, d_turned, c_raw, c_pair, acc, send_buf, landed, total,
    place_ref, rank_ref, perm_ref, mine_order, landed_orders, orders,
    local_sem, send_sem, recv_sem, order_sem, part_send, part_recv, from_below, from_above,
):
    me = lax.axis_index("pairs")
    mine = lax.axis_index("aux")
    core = lax.rem(me, CORES)
    chip = me // CORES
    chips = n // CORES
    pairs, roots, nv, width = d_ref.shape
    slots = domain_in.shape[1]
    rows = panels_ref.shape[1]
    strip = width // m
    early = complete_after(slots, pairs, 0)[-2]

    def group_of(q):
        return 0 if q < early else 1 + (q - early) // LATE


    around = sorted(range(1, chips), key=lambda k: -k.bit_count())

    def device(k, dest):
        return peer_of(chip, k, chips) * CORES + dest

    barrier = pltpu.get_barrier_semaphore()
    for k in range(chips):
        for dest in range(CORES):
            if k:
                pl.semaphore_signal(barrier, inc=1, device_id=(device(k, dest), mine), device_id_type=MESH)
    pl.semaphore_signal(barrier, inc=1, device_id=(chip * CORES + 1 - core, mine), device_id_type=MESH)

    @pl.when(mine > 0)
    def _():
        pl.semaphore_signal(barrier, inc=1, device_id=(me, mine - 1), device_id_type=MESH)

    @pl.when(mine < m - 1)
    def _():
        pl.semaphore_signal(barrier, inc=1, device_id=(me, mine + 1), device_id_type=MESH)

    small = [
        pltpu.make_async_copy(source, target, local_sem.at[4 + index])
        for index, (source, target) in enumerate(
            [(slots_in, slots_ref), (domain_in, domain_ref), (ranks_in, ranks_ref)]
        )
    ]
    for copy in small:
        copy.start()
    panels_copy = pltpu.make_async_copy(panels_ref, panels, local_sem.at[0])
    panels_copy.start()
    d_copy = pltpu.make_async_copy(d_ref, d_raw, local_sem.at[1])
    d_copy.start()
    c_copy = pltpu.make_async_copy(c_ref, c_raw, local_sem.at[2])
    c_copy.start()

    for copy in small:
        copy.wait()
    place, rank = elimination(slots_ref, slots, pairs, jnp.where(core == 0, FIXED, 0))
    for slot in range(slots):
        place_ref[slot] = place[slot]
    for pair in range(pairs):
        rank_ref[pair] = rank[pair]
    lanes = lax.broadcasted_iota(jnp.int32, (1, 128), 1)
    own_order = []
    for spot in range(slots):
        chosen = sum(jnp.where(place[slot] == spot, slot, 0) for slot in range(slots))
        own_order.append(chosen)
    line = jnp.zeros((1, 128), jnp.int32)
    for spot in range(slots):
        line = jnp.where(lanes == spot, own_order[spot], line)
    mine_order[...] = line
    for q in range(pairs):
        perm_ref[q] = sum(jnp.where(rank[pair] == q, pair, 0) for pair in range(pairs))

    beside = jnp.where(mine > 0, 1, 0) + jnp.where(mine < m - 1, 1, 0)
    pl.semaphore_wait(barrier, n - 1 + beside)

    def order_copy(peer):
        return pltpu.make_async_remote_copy(
            src_ref=mine_order,
            dst_ref=landed_orders.at[me],
            send_sem=order_sem.at[0],
            recv_sem=order_sem.at[1],
            device_id=(peer, mine),
            device_id_type=MESH,
        )

    for k in range(1, chips):
        for dest in range(CORES):
            order_copy(device(k, dest)).start()
    order_copy(chip * CORES + 1 - core).start()

    panels_copy.wait()

    def panel_copy(k, dest, spot):
        return pltpu.make_async_remote_copy(
            src_ref=outgoing.at[dest, k, spot],
            dst_ref=recv.at[spot, k * CORES + core],
            send_sem=send_sem,
            recv_sem=recv_sem.at[spot],
            device_id=(device(k, dest), mine),
            device_id_type=MESH,
        )

    def gather(dest, k, spot, ordered=True):
        peer = device(k, dest)
        slot = orders[peer, 0, spot] if ordered else spot
        outgoing[dest, k, spot] = panels[domain_ref[peer, slot]]

    def send_near(dest, spots, ordered=True):
        for spot in spots:
            gather(dest, 0, spot, ordered)

        @pl.when(core != dest)
        def _():
            for spot in spots:
                panel_copy(0, dest, spot).start()

        @pl.when(core == dest)
        def _():
            for spot in spots:
                recv[spot, dest] = outgoing[dest, 0, spot]

    def send_far(dest, spots, ordered=True):
        waiting = None
        for spot in spots:
            for k in around:
                gather(dest, k, spot, ordered)
                if waiting is not None:
                    waiting.start()
                waiting = panel_copy(k, dest, spot)
        waiting.start()

    def orders_done(sem):
        whole = landed_orders.at[pl.ds(0, n - 1)]
        pltpu.make_async_copy(whole, whole, order_sem.at[sem]).wait()

    send_far(0, range(FIXED), ordered=False)
    send_near(0, range(FIXED), ordered=False)
    landed_orders[me] = mine_order[...]
    orders_done(1)
    orders_copy = pltpu.make_async_copy(landed_orders, orders, local_sem.at[3])
    orders_copy.start()
    orders_copy.wait()
    send_far(0, range(FIXED, slots))
    for dest in range(1, CORES):
        send_far(dest, range(slots))
        send_near(dest, range(slots))
    send_near(0, range(FIXED, slots))

    for far in range(2, m):

        @pl.when((mine >= far - 1) & (mine < m - 1))
        def _():
            pl.semaphore_signal(from_below, inc=1, device_id=(me, mine + 1), device_id_type=MESH)

        @pl.when((mine <= m - far) & (mine > 0))
        def _():
            pl.semaphore_signal(from_above, inc=1, device_id=(me, mine - 1), device_id_type=MESH)

        @pl.when(mine >= far)
        def _():
            pl.semaphore_wait(from_below, 1)

        @pl.when(mine < m - far)
        def _():
            pl.semaphore_wait(from_above, 1)

    columns = lax.broadcasted_iota(jnp.int32, (1, width), 1)
    row_ids = lax.broadcasted_iota(jnp.int32, (width, 1), 0)
    d_copy.wait()
    c_copy.wait()

    def mask_pair(pair, carry):
        for root in range(roots):
            limit = ranks_ref[root, pair]
            kept = jnp.where(columns < limit, d_raw[pair, root], jnp.zeros((), d_raw.dtype))
            d_mask[pair, :, root * width:(root + 1) * width] = kept
            d_turned[pair, root * width:(root + 1) * width] = kept.T
            keep = (columns < limit) & (row_ids < limit)
            kept = jnp.where(keep, c_raw[pair, root], jnp.zeros((), c_raw.dtype))
            c_pair[pair, root, :, :width] = kept
            c_pair[pair, root, :, width:] = kept.T
        return carry

    lax.fori_loop(0, pairs, mask_pair, 0)

    def part_copy(q, owner):
        return pltpu.make_async_remote_copy(
            src_ref=send_buf.at[owner, q],
            dst_ref=landed.at[mine, q],
            send_sem=part_send,
            recv_sem=part_recv.at[group_of(q)],
            device_id=(me, owner),
            device_id_type=MESH,
        )

    def split(value):
        high = value.astype(jnp.bfloat16)
        return high, (value - high.astype(jnp.float32)).astype(jnp.bfloat16)

    def dot(left, right):
        return jnp.dot(left, right, preferred_element_type=jnp.float32)

    def compute(first, count):
        qs = [first + index for index in range(count)]
        which = [perm_ref[q] for q in qs]
        grams = [
            dot(turned[place_ref[slots_ref[0, pair]]], block[place_ref[slots_ref[1, pair]]]) for pair in which
        ]
        halves = []
        for gram, pair in zip(grams, which):
            both = dot(jnp.concatenate(split(gram), axis=0), d_mask[pair])
            halves.append(both[:nv] + both[nv:])
        wholes = []
        for half, pair in zip(halves, which):
            high, low = split(half)
            wholes.append(dot(d_turned[pair], high) + dot(d_turned[pair], low))
        kmats = [
            [whole[root * width:(root + 1) * width, root * width:(root + 1) * width] for root in range(roots)]
            for whole in wholes
        ]
        sides = [
            [dot(kmat[root].astype(jnp.bfloat16), c_pair[pair, root]) for root in range(roots)]
            for kmat, pair in zip(kmats, which)
        ]
        half = count
        for low in range(0, count, half):
            for at in range(low, min(low + half, count)):
                q = qs[at]
                for root in range(roots):
                    side = sides[at][root]
                    sigma = kmats[at][root] + side[:, :width] + side[:, width:].T
                    acc[q, root] = sigma
                    for owner in range(m):
                        send_buf[owner, q, root] = sigma[owner * strip:(owner + 1) * strip].astype(jnp.bfloat16)
            for turn in range(m - 1):
                owner = turn + jnp.where(mine <= turn, 1, 0)
                for q in qs[low:low + half]:
                    part_copy(q, owner).start()

    def take(spot):
        others = recv.at[spot, pl.ds(0, n - 1)]
        pltpu.make_async_copy(others, others, recv_sem.at[spot]).wait()
        whole = recv[spot].reshape(n * rows, nv)
        block[spot] = whole
        turned[spot] = whole.T

    def run(counts, spot):
        done = counts[spot - 1] if spot else 0
        while done < counts[spot]:
            limit = min(BATCH, early - done) if done < early else LATE - (done - early) % LATE
            step = min(limit, counts[spot] - done)
            compute(done, step)
            done += step

    for spot in range(slots):
        take(spot)

        @pl.when(core == 0)
        def _():
            run(complete_after(slots, pairs, FIXED), spot)

        @pl.when(core != 0)
        def _():
            run(complete_after(slots, pairs, 0), spot)

    gone = outgoing.at[:, pl.ds(1, chips - 1)]
    pltpu.make_async_copy(gone, gone, send_sem).wait()
    gone = outgoing.at[0, 0]
    pltpu.make_async_copy(gone, gone, send_sem).wait()

    orders_done(0)

    edges = [0, *range(early, pairs, LATE), pairs]
    for group, (low, high) in enumerate(zip(edges, edges[1:])):
        part = pl.ds(low, high - low)
        lot = landed.at[pl.ds(0, m - 1), part]
        pltpu.make_async_copy(lot, lot, part_recv.at[group]).wait()
        value = acc[part, :, pl.ds(pl.multiple_of(mine * strip, strip), strip), :]
        for offset in range(1, m):
            value = value + landed[lax.rem(mine + offset, m), part].astype(jnp.float32)
        total[part] = value.astype(total.dtype)
    for pair in range(pairs):
        out_ref[pair] = total[rank_ref[pair]]
    sent = send_buf.at[pl.ds(0, m - 1)]
    pltpu.make_async_copy(sent, sent, part_send).wait()


def per_device(n, m, panels, domain, pair_slots, ranks, transforms, trial):
    pairs, roots, nv, width = transforms.shape
    slots = domain.shape[1]
    rows = panels.shape[1]
    chips = n // CORES
    strip = width // m
    bf16 = jnp.bfloat16
    hbm = pl.BlockSpec(memory_space=pltpu.HBM)
    dma = pltpu.SemaphoreType.DMA
    return pl.pallas_call(
        functools.partial(fused_kernel, n, m),
        in_specs=[hbm] * 6,
        out_specs=pl.BlockSpec(memory_space=pltpu.VMEM),
        out_shape=pltpu.VMEM((pairs, roots, strip, width), bf16),
        scratch_shapes=[
            pltpu.SMEM(domain.shape, jnp.int32),
            pltpu.SMEM(pair_slots.shape[::-1], jnp.int32),
            pltpu.SMEM(ranks.shape[::-1], jnp.int32),
            pltpu.VMEM(panels.shape, bf16),
            pltpu.VMEM((CORES, chips, slots, rows, nv), bf16),
            pltpu.VMEM((slots, n, rows, nv), bf16),
            pltpu.VMEM((slots, n * rows, nv), bf16),
            pltpu.VMEM((slots, nv, n * rows), bf16),
            pltpu.VMEM((pairs, roots, nv, width), bf16),
            pltpu.VMEM((pairs, nv, roots * width), bf16),
            pltpu.VMEM((pairs, roots * width, nv), bf16),
            pltpu.VMEM((pairs, roots, width, width), bf16),
            pltpu.VMEM((pairs, roots, width, 2 * width), bf16),
            pltpu.VMEM((pairs, roots, width, width), jnp.float32),
            pltpu.VMEM((m, pairs, roots, strip, width), bf16),
            pltpu.VMEM((m, pairs, roots, strip, width), bf16),
            pltpu.VMEM((pairs, roots, strip, width), bf16),
            pltpu.SMEM((slots,), jnp.int32),
            pltpu.SMEM((pairs,), jnp.int32),
            pltpu.SMEM((pairs,), jnp.int32),
            pltpu.VMEM((1, 128), jnp.int32),
            pltpu.VMEM((n, 1, 128), jnp.int32),
            pltpu.SMEM((n, 1, 128), jnp.int32),
            dma((7,)),
            dma,
            dma((slots,)),
            dma((2,)),
            dma,
            dma((1 - (complete_after(slots, pairs, 0)[-2] - pairs) // LATE,)),
            pltpu.SemaphoreType.REGULAR,
            pltpu.SemaphoreType.REGULAR,
        ],
        compiler_params=pltpu.CompilerParams(
            collective_id=0, has_side_effects=True, vmem_limit_bytes=60 * 2**20
        ),
    )(domain, pair_slots.T, ranks.T, panels, transforms, trial)


def solution(mesh):
    return jax.shard_map(
        functools.partial(per_device, mesh.shape["pairs"], mesh.shape["aux"]),
        mesh=mesh,
        in_specs=(
            P(None, ("pairs", "aux"), None),
            P(),
            P("pairs", None),
            P("pairs", None),
            P("pairs", None, None, None),
            P("pairs", None, None, None),
        ),
        out_specs=P("pairs", None, "aux", None),
        check_vma=False,
    )
```

```python
import functools

import jax
import jax.numpy as jnp
from jax import lax
from jax.experimental import pallas as pl
from jax.experimental.pallas import tpu as pltpu
from jax.sharding import PartitionSpec as P

MESH = pl.DeviceIdType.MESH
CORES = 2
BATCH = 4
LATE = 4
FIXED = 2


def peer_of(me, offset, count):
    if count & (count - 1):
        return lax.rem(me + offset, count)
    peer = me
    bit = 1
    while bit < count:
        if offset & bit:
            peer = peer + bit * (1 - 2 * lax.rem(me // bit, 2))
        bit *= 2
    return peer


def complete_after(slots, pairs, fixed):
    sure = pairs
    counts = [pairs]
    for left in range(slots, 1, -1):
        sure -= min(sure, 2 * sure // (left - fixed)) if left > fixed else sure
        counts.insert(0, sure)
    return counts


def elimination(slots_ref, slots, pairs, fixed):
    bits = (pairs + 1).bit_length()
    fields = 31 // bits
    words = -(-slots // fields)

    def shift_of(slot, word):
        shift = slot - word * fields
        inside = (shift >= 0) & (shift < fields) if words > 1 else True
        return jnp.where(inside, shift, 0) * bits, inside

    def mark(slot, word):
        shift, inside = shift_of(slot, word)
        return jnp.where(inside, jnp.left_shift(1, shift), 0)

    marks = [
        [mark(slots_ref[0, p], w) | mark(slots_ref[1, p], w) for w in range(words)] for p in range(pairs)
    ]
    place = [jnp.int32(0)] * slots
    extra = [jnp.maximum(fixed - slot, 0) * 2**bits for slot in range(slots)]
    for spot in range(slots - 1, 0, -1):
        totals = [sum(marks[p][w] for p in range(pairs)) for w in range(words)]
        best, pick = None, jnp.int32(0)
        for slot in range(slots):
            count = ((totals[slot // fields] >> (bits * (slot % fields))) & (2**bits - 1)) + extra[slot]
            if best is None:
                best = count
            else:
                less = count < best
                best = jnp.where(less, count, best)
                pick = jnp.where(less, slot, pick)
        for slot in range(slots):
            hit = pick == slot
            place[slot] = jnp.where(hit, spot, place[slot])
            extra[slot] = jnp.where(hit, (slots + 1) * 2**bits, extra[slot])
        for p in range(pairs):
            gone = 0
            for w in range(words):
                shift, inside = shift_of(pick, w)
                gone = gone | jnp.where(inside, (marks[p][w] >> shift) & 1, 0)
            marks[p] = [value & (gone - 1) for value in marks[p]]
    return place


def ranking(stages):
    rank = [jnp.int32(0)] * len(stages)
    for p in range(len(stages)):
        for q in range(p + 1, len(stages)):
            later = jnp.where(stages[p] > stages[q], 1, 0)
            rank[p] = rank[p] + later
            rank[q] = rank[q] + 1 - later
    return rank


def fused_kernel(
    n, m, domain_in, slots_in, ranks_in, panels_ref, d_ref, c_ref, out_ref,
    domain_ref, slots_ref, ranks_ref,
    panels, outgoing, recv, block, turned, d_raw, d_mask, d_turned, c_raw, c_pair, acc, send_buf, landed, total,
    place_ref, rank_ref, perm_ref, mine_order, landed_orders, orders,
    local_sem, send_sem, recv_sem, order_sem, part_send, part_recv, from_below, from_above,
):
    me = lax.axis_index("pairs")
    mine = lax.axis_index("aux")
    core = lax.rem(me, CORES)
    chip = me // CORES
    chips = n // CORES
    pairs, roots, nv, width = d_ref.shape
    slots = domain_in.shape[1]
    rows = panels_ref.shape[1]
    strip = width // m
    early = complete_after(slots, pairs, 0)[-2]

    def group_of(q):
        return 0 if q < early else 1 + (q - early) // LATE


    around = sorted(range(1, chips), key=lambda k: -k.bit_count())

    def device(k, dest):
        return peer_of(chip, k, chips) * CORES + dest

    barrier = pltpu.get_barrier_semaphore()
    for k in range(chips):
        for dest in range(CORES):
            if k:
                pl.semaphore_signal(barrier, inc=1, device_id=(device(k, dest), mine), device_id_type=MESH)
    pl.semaphore_signal(barrier, inc=1, device_id=(chip * CORES + 1 - core, mine), device_id_type=MESH)

    @pl.when(mine > 0)
    def _():
        pl.semaphore_signal(barrier, inc=1, device_id=(me, mine - 1), device_id_type=MESH)

    @pl.when(mine < m - 1)
    def _():
        pl.semaphore_signal(barrier, inc=1, device_id=(me, mine + 1), device_id_type=MESH)

    small = [
        pltpu.make_async_copy(source, target, local_sem.at[4 + index])
        for index, (source, target) in enumerate(
            [(slots_in, slots_ref), (domain_in, domain_ref), (ranks_in, ranks_ref)]
        )
    ]
    for copy in small:
        copy.start()
    panels_copy = pltpu.make_async_copy(panels_ref, panels, local_sem.at[0])
    panels_copy.start()
    d_copy = pltpu.make_async_copy(d_ref, d_raw, local_sem.at[1])
    d_copy.start()
    c_copy = pltpu.make_async_copy(c_ref, c_raw, local_sem.at[2])
    c_copy.start()

    for copy in small:
        copy.wait()
    place = elimination(slots_ref, slots, pairs, jnp.where(core == 0, FIXED, 0))
    for slot in range(slots):
        place_ref[slot] = place[slot]
    lanes = lax.broadcasted_iota(jnp.int32, (1, 128), 1)
    own_order = []
    for spot in range(slots):
        chosen = sum(jnp.where(place[slot] == spot, slot, 0) for slot in range(slots))
        own_order.append(chosen)
    line = jnp.zeros((1, 128), jnp.int32)
    for spot in range(slots):
        line = jnp.where(lanes == spot, own_order[spot], line)
    mine_order[...] = line
    beside = jnp.where(mine > 0, 1, 0) + jnp.where(mine < m - 1, 1, 0)
    pl.semaphore_wait(barrier, n - 1 + beside)

    def order_copy(peer):
        return pltpu.make_async_remote_copy(
            src_ref=mine_order,
            dst_ref=landed_orders.at[me],
            send_sem=order_sem.at[0],
            recv_sem=order_sem.at[1],
            device_id=(peer, mine),
            device_id_type=MESH,
        )

    for k in range(1, chips):
        for dest in range(CORES):
            order_copy(device(k, dest)).start()
    order_copy(chip * CORES + 1 - core).start()

    panels_copy.wait()

    def panel_copy(k, dest, spot):
        return pltpu.make_async_remote_copy(
            src_ref=outgoing.at[dest, k, spot],
            dst_ref=recv.at[spot, k * CORES + core],
            send_sem=send_sem,
            recv_sem=recv_sem.at[spot],
            device_id=(device(k, dest), mine),
            device_id_type=MESH,
        )

    def gather(dest, k, spot, ordered=True):
        peer = device(k, dest)
        slot = orders[peer, 0, spot] if ordered else spot
        outgoing[dest, k, spot] = panels[domain_ref[peer, slot]]

    def send_near(dest, spots, ordered=True):
        for spot in spots:
            gather(dest, 0, spot, ordered)

        @pl.when(core != dest)
        def _():
            for spot in spots:
                panel_copy(0, dest, spot).start()

        @pl.when(core == dest)
        def _():
            for spot in spots:
                recv[spot, dest] = outgoing[dest, 0, spot]

    def send_far(dest, spots, ordered=True):
        waiting = None
        for spot in spots:
            for k in around:
                gather(dest, k, spot, ordered)
                if waiting is not None:
                    waiting.start()
                waiting = panel_copy(k, dest, spot)
        waiting.start()

    def orders_done(sem):
        whole = landed_orders.at[pl.ds(0, n - 1)]
        pltpu.make_async_copy(whole, whole, order_sem.at[sem]).wait()

    send_far(0, range(FIXED), ordered=False)
    send_near(0, range(FIXED), ordered=False)
    landed_orders[me] = mine_order[...]
    orders_done(1)
    orders_copy = pltpu.make_async_copy(landed_orders, orders, local_sem.at[3])
    orders_copy.start()
    orders_copy.wait()
    send_far(0, range(FIXED, slots))
    for dest in range(1, CORES):
        send_far(dest, range(slots))
        send_near(dest, range(slots))
    send_near(0, range(FIXED, slots))

    rank = ranking(
        [
            jnp.maximum(place_ref[slots_ref[0, pair]], place_ref[slots_ref[1, pair]])
            for pair in range(pairs)
        ]
    )
    for pair in range(pairs):
        rank_ref[pair] = rank[pair]
    for q in range(pairs):
        perm_ref[q] = sum(jnp.where(rank[pair] == q, pair, 0) for pair in range(pairs))

    for far in range(2, m):

        @pl.when((mine >= far - 1) & (mine < m - 1))
        def _():
            pl.semaphore_signal(from_below, inc=1, device_id=(me, mine + 1), device_id_type=MESH)

        @pl.when((mine <= m - far) & (mine > 0))
        def _():
            pl.semaphore_signal(from_above, inc=1, device_id=(me, mine - 1), device_id_type=MESH)

        @pl.when(mine >= far)
        def _():
            pl.semaphore_wait(from_below, 1)

        @pl.when(mine < m - far)
        def _():
            pl.semaphore_wait(from_above, 1)

    columns = lax.broadcasted_iota(jnp.int32, (1, width), 1)
    row_ids = lax.broadcasted_iota(jnp.int32, (width, 1), 0)
    d_copy.wait()
    c_copy.wait()

    def mask_pair(pair, carry):
        for root in range(roots):
            limit = ranks_ref[root, pair]
            kept = jnp.where(columns < limit, d_raw[pair, root], jnp.zeros((), d_raw.dtype))
            d_mask[pair, :, root * width:(root + 1) * width] = kept
            d_turned[pair, root * width:(root + 1) * width] = kept.T
            keep = (columns < limit) & (row_ids < limit)
            kept = jnp.where(keep, c_raw[pair, root], jnp.zeros((), c_raw.dtype))
            c_pair[pair, root, :, :width] = kept
            c_pair[pair, root, :, width:] = kept.T
        return carry

    lax.fori_loop(0, pairs, mask_pair, 0)

    def part_copy(q, owner):
        return pltpu.make_async_remote_copy(
            src_ref=send_buf.at[owner, q],
            dst_ref=landed.at[mine, q],
            send_sem=part_send,
            recv_sem=part_recv.at[group_of(q)],
            device_id=(me, owner),
            device_id_type=MESH,
        )

    def split(value):
        high = value.astype(jnp.bfloat16)
        return high, (value - high.astype(jnp.float32)).astype(jnp.bfloat16)

    def dot(left, right):
        return jnp.dot(left, right, preferred_element_type=jnp.float32)

    def compute(first, count):
        qs = [first + index for index in range(count)]
        which = [perm_ref[q] for q in qs]
        grams = [
            dot(turned[place_ref[slots_ref[0, pair]]], block[place_ref[slots_ref[1, pair]]]) for pair in which
        ]
        halves = []
        for gram, pair in zip(grams, which):
            both = dot(jnp.concatenate(split(gram), axis=0), d_mask[pair])
            halves.append(both[:nv] + both[nv:])
        wholes = []
        for half, pair in zip(halves, which):
            high, low = split(half)
            wholes.append(dot(d_turned[pair], high) + dot(d_turned[pair], low))
        kmats = [
            [whole[root * width:(root + 1) * width, root * width:(root + 1) * width] for root in range(roots)]
            for whole in wholes
        ]
        sides = [
            [dot(kmat[root].astype(jnp.bfloat16), c_pair[pair, root]) for root in range(roots)]
            for kmat, pair in zip(kmats, which)
        ]
        for q, kmat, side in zip(qs, kmats, sides):
            for root in range(roots):
                sigma = kmat[root] + side[root][:, :width] + side[root][:, width:].T
                acc[q, root] = sigma
                for owner in range(m):
                    send_buf[owner, q, root] = sigma[owner * strip:(owner + 1) * strip].astype(jnp.bfloat16)
        for turn in range(m - 1):
            owner = turn + jnp.where(mine <= turn, 1, 0)
            for q in qs:
                part_copy(q, owner).start()

    def take(spot):
        others = recv.at[spot, pl.ds(0, n - 1)]
        pltpu.make_async_copy(others, others, recv_sem.at[spot]).wait()
        whole = recv[spot].reshape(n * rows, nv)
        block[spot] = whole
        turned[spot] = whole.T

    def run(counts, spot):
        done = counts[spot - 1] if spot else 0
        while done < counts[spot]:
            limit = min(BATCH, early - done) if done < early else LATE - (done - early) % LATE
            step = min(limit, counts[spot] - done)
            compute(done, step)
            done += step

    for spot in range(slots):
        take(spot)

        @pl.when(core == 0)
        def _():
            run(complete_after(slots, pairs, FIXED), spot)

        @pl.when(core != 0)
        def _():
            run(complete_after(slots, pairs, 0), spot)

    gone = outgoing.at[:, pl.ds(1, chips - 1)]
    pltpu.make_async_copy(gone, gone, send_sem).wait()
    gone = outgoing.at[0, 0]
    pltpu.make_async_copy(gone, gone, send_sem).wait()

    orders_done(0)

    edges = [0, *range(early, pairs, LATE), pairs]
    for group, (low, high) in enumerate(zip(edges, edges[1:])):
        part = pl.ds(low, high - low)
        lot = landed.at[pl.ds(0, m - 1), part]
        pltpu.make_async_copy(lot, lot, part_recv.at[group]).wait()
        value = acc[part, :, pl.ds(pl.multiple_of(mine * strip, strip), strip), :]
        for offset in range(1, m):
            value = value + landed[lax.rem(mine + offset, m), part].astype(jnp.float32)
        total[part] = value.astype(total.dtype)
    for pair in range(pairs):
        out_ref[pair] = total[rank_ref[pair]]
    sent = send_buf.at[pl.ds(0, m - 1)]
    pltpu.make_async_copy(sent, sent, part_send).wait()


def per_device(n, m, panels, domain, pair_slots, ranks, transforms, trial):
    pairs, roots, nv, width = transforms.shape
    slots = domain.shape[1]
    rows = panels.shape[1]
    chips = n // CORES
    strip = width // m
    bf16 = jnp.bfloat16
    hbm = pl.BlockSpec(memory_space=pltpu.HBM)
    dma = pltpu.SemaphoreType.DMA
    return pl.pallas_call(
        functools.partial(fused_kernel, n, m),
        in_specs=[hbm] * 6,
        out_specs=pl.BlockSpec(memory_space=pltpu.VMEM),
        out_shape=pltpu.VMEM((pairs, roots, strip, width), bf16),
        scratch_shapes=[
            pltpu.SMEM(domain.shape, jnp.int32),
            pltpu.SMEM(pair_slots.shape[::-1], jnp.int32),
            pltpu.SMEM(ranks.shape[::-1], jnp.int32),
            pltpu.VMEM(panels.shape, bf16),
            pltpu.VMEM((CORES, chips, slots, rows, nv), bf16),
            pltpu.VMEM((slots, n, rows, nv), bf16),
            pltpu.VMEM((slots, n * rows, nv), bf16),
            pltpu.VMEM((slots, nv, n * rows), bf16),
            pltpu.VMEM((pairs, roots, nv, width), bf16),
            pltpu.VMEM((pairs, nv, roots * width), bf16),
            pltpu.VMEM((pairs, roots * width, nv), bf16),
            pltpu.VMEM((pairs, roots, width, width), bf16),
            pltpu.VMEM((pairs, roots, width, 2 * width), bf16),
            pltpu.VMEM((pairs, roots, width, width), jnp.float32),
            pltpu.VMEM((m, pairs, roots, strip, width), bf16),
            pltpu.VMEM((m, pairs, roots, strip, width), bf16),
            pltpu.VMEM((pairs, roots, strip, width), bf16),
            pltpu.SMEM((slots,), jnp.int32),
            pltpu.SMEM((pairs,), jnp.int32),
            pltpu.SMEM((pairs,), jnp.int32),
            pltpu.VMEM((1, 128), jnp.int32),
            pltpu.VMEM((n, 1, 128), jnp.int32),
            pltpu.SMEM((n, 1, 128), jnp.int32),
            dma((7,)),
            dma,
            dma((slots,)),
            dma((2,)),
            dma,
            dma((1 - (complete_after(slots, pairs, 0)[-2] - pairs) // LATE,)),
            pltpu.SemaphoreType.REGULAR,
            pltpu.SemaphoreType.REGULAR,
        ],
        compiler_params=pltpu.CompilerParams(
            collective_id=0, has_side_effects=True, vmem_limit_bytes=60 * 2**20
        ),
    )(domain, pair_slots.T, ranks.T, panels, transforms, trial)


def solution(mesh):
    return jax.shard_map(
        functools.partial(per_device, mesh.shape["pairs"], mesh.shape["aux"]),
        mesh=mesh,
        in_specs=(
            P(None, ("pairs", "aux"), None),
            P(),
            P("pairs", None),
            P("pairs", None),
            P("pairs", None, None, None),
            P("pairs", None, None, None),
        ),
        out_specs=P("pairs", None, "aux", None),
        check_vma=False,
    )
```
